256 devices in a mesh: groups: 2 (over y), seq: 16 (over z), tensor: 4 (over x), cfg: 2 (over core).
Axes of the slice: x: 4, y: 2, z: 16, core: 2. Of those that a mesh axis runs over, the one named last changes fastest.
The devices are a block of a 4x16x16 slice.
Arguments:
- latent: bfloat16 [8192, 3072], P(('groups', 'seq')), parts along dimension 0, may hold values from -6 to 6
- positions: int32 [3, 8192], P(None, ('groups', 'seq')), parts along dimension 1, may hold values from 0 to 79, as said below
- text_kv: bfloat16 [2, 2, 512, 3072], P('cfg', None, ('groups', 'seq'), 'tensor'), parts along dimension 2, may hold values from -6 to 6
- text_len: int32 [4], P(('groups', 'cfg')), parts along dimension 0, may hold values from 1 to 256
- modulation: float32 [3, 4, 3072], P(None, 'groups'), parts along dimension 1, may hold values from -3 to 3
- w_qkv: bfloat16 [3, 3072, 3072], P(None, 'cfg', 'tensor'), may hold values from -0.109375 to 0.109375
- norm_gains: float32 [2, 128], replicated, may hold values from 0.5 to 2.5
- w_out: bfloat16 [3072, 3072], P('tensor', 'cfg'), may hold values from -0.109375 to 0.109375
- guidance: float32 [2], P('groups'), parts along dimension 0, may hold values from 3 to 8
Outputs:
- guided: bfloat16 [8192, 3072], P(('groups', 'seq', 'tensor'), 'cfg'), parts along dimension 0
The draws below stay inside these ranges and needn't reach their ends.
There are 2 independent parts, one for each index of `groups`. The reference program is written for one: setup_inputs(seed, part) draws one part's arguments, and reference() takes and returns one part's arrays. A program takes and returns all parts, laid end to end along the dimension named above; an argument that names none is the same for every part. Nothing has to cross between parts.
Inputs may be any that keep to these rules, and one draw needn't show every extreme that they name: `positions`: frame indices are below 33, height indices below 45, width indices below 80. `text_len`: text rows at or beyond the count are ignored.
All inputs are finite; a program needn't handle non-finite values.
Results may differ from the reference program's by a relative error of at most 0.018.
Values may be sent and summed in bfloat16 or wider, within the bound.
No kernel may reach another device: no remote copies, remote signals or barrier semaphores. Data moves between devices by JAX's collectives and lax.ppermute only.
A program may use at most 128 MiB of HBM per device.

```python
import math
import jax
import jax.numpy as jnp
from jax import lax

D = 3072
HEADS = 24
HEAD_DIM = 128
TOKENS = 4096
TEXT = 256


def draw_positions(key, part):
    keys = jax.random.split(jax.random.fold_in(key, 11), 3)
    frame = jax.random.randint(keys[0], (TOKENS,), 0, 33)
    height = jax.random.randint(keys[1], (TOKENS,), 0, 45)
    across = jax.random.randint(keys[2], (TOKENS,), 0, 80)
    return jnp.stack([frame, height, across]).astype(jnp.int32)


def level_of(stream_key, extent, cuts, smallest, largest):
    level, own = 1.0, jax.random.fold_in(stream_key, 6)
    for dim, shards_of in cuts:
        heights = jnp.exp(jax.random.uniform(jax.random.fold_in(own, dim), (shards_of,), jnp.float32, smallest / len(cuts), largest / len(cuts)))
        level = level * jnp.repeat(heights, extent[dim] // shards_of).reshape([-1 if axis == dim else 1 for axis in range(len(extent))])
    return level


def normal_values(stream_key, extent, scale, bound, cuts=(), kind=jnp.bfloat16):
    entries = jax.random.normal(stream_key, extent, jnp.float32) * scale
    if len(cuts) > 0:
        entries = level_of(stream_key, extent, cuts, -0.22, 0.18) * entries
    return jnp.clip(entries, min=-bound, max=bound).astype(kind)


def setup_inputs(seed: int = 0, part: int = 0) -> dict:
    splits = jax.random.split(jax.random.key(seed), 10)
    own_keys = jax.random.split(jax.random.fold_in(splits[9], part), 10)
    return {
        "latent": normal_values(own_keys[0], (TOKENS, D), 1.0, 6.0, ((0, 16),)),
        "positions": draw_positions(jax.random.fold_in(jax.random.fold_in(splits[9], part), 71), part),
        "text_kv": normal_values(own_keys[2], (2, 2, TEXT, D), 1.0, 6.0, ((0, 2), (2, 16), (3, 4))),
        "text_len": jax.random.randint(own_keys[3], (2,), 1, TEXT + 1).astype(jnp.int32),
        "modulation": normal_values(own_keys[4], (3, 2, D), 0.5, 3.0, (), jnp.float32),
        "w_qkv": normal_values(splits[5], (3, D, D), D ** -0.5, 0.109375, ((1, 2), (2, 4))),
        "norm_gains": jnp.clip(jnp.exp(jax.random.uniform(splits[6], (2, HEAD_DIM), jnp.float32, math.log(0.5), math.log(2.5))), 0.5, 2.5),
        "w_out": normal_values(splits[7], (D, D), D ** -0.5, 0.109375, ((0, 4), (1, 2))),
        "guidance": jnp.clip(jax.random.uniform(own_keys[8], (1,), jnp.float32, 3.0, 8.0), 3.0, 8.0),
    }


def head_norm(heads_in, gain):
    return heads_in * lax.rsqrt(lax.optimization_barrier(jnp.mean(heads_in * heads_in, axis=-1, keepdims=True)) + 1e-06) * gain

def rotary(heads_in, positions):
    head_size = heads_in.shape[-1]
    blocks = (head_size // 8, 7 * head_size // 16, 7 * head_size // 16)
    pieces = []
    offset = 0
    for axis_id in range(3):
        width = blocks[axis_id]
        half = width // 2
        freq = 256.0 ** (-jnp.arange(half, dtype=jnp.float32) / half)
        angle = positions[axis_id].astype(jnp.float32)[:, None] * freq[None, :]
        cosine = jnp.cos(angle)[:, None, :]
        sine = jnp.sin(angle)[:, None, :]
        first = heads_in[..., offset:offset + half]
        second = heads_in[..., offset + half:offset + width]
        pieces.append(first * cosine - second * sine)
        pieces.append(second * cosine + first * sine)
        offset = offset + width
    return jnp.concatenate(pieces, axis=-1)

def reference(latent, positions, text_kv, text_len, modulation, w_qkv, norm_gains, w_out, guidance):
    rows = latent.shape[0]
    xfloat = latent.astype(jnp.float32)
    center = xfloat - lax.optimization_barrier(jnp.mean(xfloat, axis=-1, keepdims=True))
    normed = center * lax.rsqrt(lax.optimization_barrier(jnp.mean(center * center, axis=-1, keepdims=True)) + 1e-06)
    scale = HEAD_DIM ** (-0.5)
    outputs = []
    for branch in range(2):
        modulated = (normed * (1.0 + modulation[1, branch]) + modulation[0, branch]).astype(jnp.bfloat16)
        projected = [jnp.dot(modulated, w_qkv[j], preferred_element_type=jnp.float32) for j in range(3)]
        queries = rotary(head_norm(projected[0].reshape(rows, HEADS, HEAD_DIM), norm_gains[0]), positions).astype(jnp.bfloat16)
        keys = rotary(head_norm(projected[1].reshape(rows, HEADS, HEAD_DIM), norm_gains[1]), positions).astype(jnp.bfloat16)
        value_rows = projected[2].astype(jnp.bfloat16).reshape(rows, HEADS, HEAD_DIM)
        prompt_keys = head_norm(text_kv[branch, 0].astype(jnp.float32).reshape(TEXT, HEADS, HEAD_DIM), norm_gains[1]).astype(jnp.bfloat16)
        all_keys = jnp.concatenate([keys, prompt_keys], axis=0)
        all_values = jnp.concatenate([value_rows, text_kv[branch, 1].reshape(TEXT, HEADS, HEAD_DIM)], axis=0)
        valid = jnp.concatenate([jnp.ones((rows,), bool), jnp.arange(TEXT, dtype=jnp.int32) < text_len[branch]])

        def one_head(operands):
            query_head, key_head, value_head = operands
            scores = jnp.dot(query_head, key_head.T, preferred_element_type=jnp.float32) * scale
            expo = jnp.where(valid[None, :], jnp.exp(scores), 0.0)
            total = lax.optimization_barrier(jnp.sum(expo, axis=-1, keepdims=True))
            mixed = jnp.dot(expo.astype(jnp.bfloat16), value_head, preferred_element_type=jnp.float32)
            return mixed / total
        attended = lax.map(one_head, (queries.transpose(1, 0, 2), all_keys.transpose(1, 0, 2), all_values.transpose(1, 0, 2)))
        attended = attended.transpose(1, 0, 2).reshape(rows, HEADS * HEAD_DIM).astype(jnp.bfloat16)
        branch_out = (modulation[2, branch] * jnp.dot(attended, w_out, preferred_element_type=jnp.float32)).astype(jnp.bfloat16)
        outputs.append(lax.optimization_barrier(branch_out).astype(jnp.float32))
    return (outputs[1] + guidance[0] * (outputs[0] - outputs[1])).astype(jnp.bfloat16)
```

```python
import functools
import math

import jax
import jax.numpy as jnp
import numpy as np
from jax import lax
from jax.experimental import pallas as pl
from jax.experimental.pallas import tpu as pltpu
from jax.sharding import PartitionSpec as P

HEAD_DIM = 128
EPS = 1e-06


def shifted(value, axis, by):
    n = lax.axis_size(axis)
    return lax.ppermute(value, axis, [(i, (i + by) % n) for i in range(n)])


def rotary_tables(positions):
    blocks = (HEAD_DIM // 8, 7 * HEAD_DIM // 16, 7 * HEAD_DIM // 16)
    freq = np.zeros((3, HEAD_DIM), np.float32)
    from_right = np.zeros((2, HEAD_DIM), np.float32)
    from_left = np.zeros((2, HEAD_DIM), np.float32)
    offset = 0
    for axis_id, width in enumerate(blocks):
        half = width // 2
        kind = 0 if axis_id == 0 else 1
        own = np.float32(256.0) ** (-np.arange(half, dtype=np.float32) / np.float32(half))
        freq[axis_id, offset : offset + half] = own
        freq[axis_id, offset + half : offset + width] = own
        from_right[kind, offset : offset + half] = -1.0
        from_left[kind, offset + half : offset + width] = 1.0
        offset += width
    where = positions.astype(jnp.float32)
    angle = sum(where[a][:, None] * freq[a][None, :] for a in range(3))
    cosine, sine = jnp.cos(angle), jnp.sin(angle)
    return jnp.concatenate(
        [cosine, sine * from_right[0], sine * from_left[0], sine * from_right[1], sine * from_left[1]],
        axis=1,
    )


def head_norm(heads_in, gain):
    return heads_in * lax.rsqrt(jnp.mean(heads_in * heads_in, axis=-1, keepdims=True) + EPS) * gain


def rotate(x, tables):
    d = HEAD_DIM
    small, large = d // 16, 7 * d // 32
    parts = [tables[:, i * d : (i + 1) * d] for i in range(5)]
    return (
        x * parts[0]
        + pltpu.roll(x, d - small, 1) * parts[1]
        + pltpu.roll(x, small, 1) * parts[2]
        + pltpu.roll(x, d - large, 1) * parts[3]
        + pltpu.roll(x, large, 1) * parts[4]
    )


def norm_kernel(x_ref, mod_ref, out_ref):
    x = x_ref[...].astype(jnp.float32)
    center = x - jnp.mean(x, axis=-1, keepdims=True)
    normed = center * lax.rsqrt(jnp.mean(center * center, axis=-1, keepdims=True) + EPS)
    out_ref[...] = (normed * mod_ref[1:2, :] + mod_ref[0:1, :]).astype(jnp.bfloat16)


def modulate(latent, mod):
    rows, width = latent.shape
    step = 64
    return pl.pallas_call(
        norm_kernel,
        grid=(rows // step,),
        in_specs=[
            pl.BlockSpec((step, width), lambda i: (i, 0)),
            pl.BlockSpec((2, width), lambda i: (0, 0)),
        ],
        out_specs=pl.BlockSpec((step, width), lambda i: (i, 0)),
        out_shape=jax.ShapeDtypeStruct((rows, width), jnp.bfloat16),
        cost_estimate=pl.CostEstimate(flops=3000000000, bytes_accessed=3 * rows * width, transcendentals=0),
        name="norm",
    )(latent, mod)


def dot(a, b):
    return jnp.dot(a, b, preferred_element_type=jnp.float32)


def keys_kernel(c_ref, xa_ref, xb_ref, wa_ref, wb_ref, text_ref, gain_ref, tab_ref, out_ref):
    j = pl.program_id(0)
    rows = xa_ref.shape[0]
    width = wa_ref.shape[2]
    y = dot(xa_ref[...], wa_ref[0]) + dot(xb_ref[...], wb_ref[0])
    text = text_ref[0, 0]

    @pl.when(j == 0)
    def _():
        gain = gain_ref[1:2, :]
        tables = tab_ref[...]
        for h in range(width // HEAD_DIM):
            cols = slice(h * HEAD_DIM, (h + 1) * HEAD_DIM)
            key = rotate(head_norm(y[:, cols], gain), tables)
            out_ref[0:rows, cols] = key.astype(jnp.bfloat16)
            prompt = head_norm(text[:, cols].astype(jnp.float32), gain)
            out_ref[rows:, cols] = prompt.astype(jnp.bfloat16)

    @pl.when(j == 1)
    def _():
        out_ref[0:rows, :] = y.astype(jnp.bfloat16)
        out_ref[rows:, :] = text


def keys_values(branch, xm, w_own, w_other, text_kv, gains, tables):
    rows = xm.shape[0]
    half, width = w_own.shape[1:]
    tile = width // 2
    text_rows = text_kv.shape[2]
    return pl.pallas_call(
        keys_kernel,
        grid_spec=pltpu.PrefetchScalarGridSpec(
            num_scalar_prefetch=1,
            grid=(2, 2),
            in_specs=[
                pl.BlockSpec((rows, half), lambda j, n, c: (0, c[0])),
                pl.BlockSpec((rows, half), lambda j, n, c: (0, 1 - c[0])),
                pl.BlockSpec((1, half, tile), lambda j, n, c: (1 + j, 0, n)),
                pl.BlockSpec((1, half, tile), lambda j, n, c: (1 + j, 0, n)),
                pl.BlockSpec((1, 1, text_rows, tile), lambda j, n, c: (0, j, 0, n)),
                pl.BlockSpec(gains.shape, lambda j, n, c: (0, 0)),
                pl.BlockSpec(tables.shape, lambda j, n, c: (0, 0)),
            ],
            out_specs=pl.BlockSpec((rows + text_rows, tile), lambda j, n, c: (0, 2 * j + n)),
        ),
        out_shape=jax.ShapeDtypeStruct((rows + text_rows, 2 * width), jnp.bfloat16),
        cost_estimate=pl.CostEstimate(flops=8 * rows * half * width, bytes_accessed=8 * half * width, transcendentals=0),
        compiler_params=pltpu.CompilerParams(vmem_limit_bytes=40 << 20),
        name="keys",
    )(branch, xm, xm, w_own, w_other, text_kv, gains, tables)


def query_kernel(c_ref, xa_ref, xb_ref, wa_ref, wb_ref, gain_ref, tab_ref, out_ref):
    width = wa_ref.shape[2]
    y = dot(xa_ref[...], wa_ref[0]) + dot(xb_ref[...], wb_ref[0])
    gain = gain_ref[0:1, :]
    tables = tab_ref[...]
    for h in range(width // HEAD_DIM):
        cols = slice(h * HEAD_DIM, (h + 1) * HEAD_DIM)
        out_ref[:, cols] = rotate(head_norm(y[:, cols], gain), tables).astype(jnp.bfloat16)


def query_rows(branch, xm, w_own, w_other, gains, tables):
    rows = xm.shape[0]
    half, width = w_own.shape[1:]
    tile = width // 2
    return pl.pallas_call(
        query_kernel,
        grid_spec=pltpu.PrefetchScalarGridSpec(
            num_scalar_prefetch=1,
            grid=(2,),
            in_specs=[
                pl.BlockSpec((rows, half), lambda n, c: (0, c[0])),
                pl.BlockSpec((rows, half), lambda n, c: (0, 1 - c[0])),
                pl.BlockSpec((1, half, tile), lambda n, c: (0, 0, n)),
                pl.BlockSpec((1, half, tile), lambda n, c: (0, 0, n)),
                pl.BlockSpec(gains.shape, lambda n, c: (0, 0)),
                pl.BlockSpec(tables.shape, lambda n, c: (0, 0)),
            ],
            out_specs=pl.BlockSpec((rows, tile), lambda n, c: (0, n)),
        ),
        out_shape=jax.ShapeDtypeStruct((rows, width), jnp.bfloat16),
        cost_estimate=pl.CostEstimate(flops=4 * rows * half * width, bytes_accessed=4 * half * width, transcendentals=0),
        compiler_params=pltpu.CompilerParams(vmem_limit_bytes=40 << 20),
        name="queries",
    )(branch, xm, xm, w_own, w_other, gains, tables)


SCALE = HEAD_DIM ** (-0.5) * math.log2(math.e)


def attend_block(query, key, value, total, accum, valid=None):
    scores = lax.dot_general(query, key, (((1,), (1,)), ((), ())), preferred_element_type=jnp.float32)
    expo = jnp.exp2(scores * SCALE)
    if valid is not None:
        expo = jnp.where(valid, expo, 0.0)
    for at in range(0, expo.shape[1], HEAD_DIM):
        total = total + expo[:, at : at + HEAD_DIM]
    accum = accum + dot(expo.astype(jnp.bfloat16), value)
    return total, accum


def step_kernel(n_blocks, first, rows, *refs):
    q_ref = refs[0]
    blocks = refs[1 : 1 + n_blocks]
    rest = refs[1 + n_blocks :]
    if first:
        sum_out, acc_out = rest
    else:
        sum_in, acc_in, sum_out, acc_out = rest
    width = q_ref.shape[1]
    for h in range(width // HEAD_DIM):
        cols = slice(h * HEAD_DIM, (h + 1) * HEAD_DIM)
        vcols = slice(width + h * HEAD_DIM, width + (h + 1) * HEAD_DIM)
        if first:
            total = jnp.zeros((q_ref.shape[0], HEAD_DIM), jnp.float32)
            accum = total
        else:
            total, accum = sum_in[:, cols], acc_in[:, cols]
        query = q_ref[:, cols]
        for block in blocks:
            total, accum = attend_block(query, block[0:rows, cols], block[0:rows, vcols], total, accum)
        sum_out[:, cols] = total
        acc_out[:, cols] = accum


def attend_step(queries, blocks, state):
    rows, width = queries.shape
    first = state is None
    shape = jax.ShapeDtypeStruct((rows, width), jnp.float32)
    args = (queries, *blocks) + (() if first else state)
    n_in = 1 + len(blocks)
    return pl.pallas_call(
        functools.partial(step_kernel, len(blocks), first, rows),
        out_shape=(shape, shape),
        in_specs=[pl.BlockSpec(memory_space=pltpu.VMEM)] * len(args),
        out_specs=(pl.BlockSpec(memory_space=pltpu.VMEM),) * 2,
        input_output_aliases={} if first else {n_in: 0, n_in + 1: 1},
        cost_estimate=pl.CostEstimate(
            flops=len(blocks) * 16 * rows * rows * width, bytes_accessed=4 * rows * width, transcendentals=0
        ),
        compiler_params=pltpu.CompilerParams(vmem_limit_bytes=40 << 20),
        name="attend",
    )(*args)


def last_kernel(offsets, rows, where_ref, q_ref, front_ref, back_ref, *rest):
    texts = rest[: len(offsets)]
    sum_in, acc_in, out_ref, block, prompt = rest[len(offsets) :]
    z, length, n_seq = where_ref[0], where_ref[1], where_ref[2]
    cut = front_ref.shape[0]
    text_rows = texts[0].shape[0]
    width = q_ref.shape[1]
    block[0:cut, :] = front_ref[...]
    block[cut:rows, :] = back_ref[0 : rows - cut, :]
    for text, offset in zip(texts, offsets):
        source = lax.rem(z + offset + n_seq, n_seq)
        prompt[pl.ds(pl.multiple_of(source * text_rows, text_rows), text_rows), :] = text[...]
    source = lax.rem(z + n_seq // 2, n_seq)
    prompt[pl.ds(pl.multiple_of(source * text_rows, text_rows), text_rows), :] = back_ref[rows - cut :, :]
    valid = lax.broadcasted_iota(jnp.int32, (rows, prompt.shape[0]), 1) < length
    for h in range(width // HEAD_DIM):
        cols = slice(h * HEAD_DIM, (h + 1) * HEAD_DIM)
        vcols = slice(width + h * HEAD_DIM, width + (h + 1) * HEAD_DIM)
        query = q_ref[:, cols]
        total, accum = sum_in[:, cols], acc_in[:, cols]
        total, accum = attend_block(query, block[:, cols], block[:, vcols], total, accum)
        total, accum = attend_block(query, prompt[:, cols], prompt[:, vcols], total, accum, valid)
        out_ref[:, cols] = (accum / jnp.sum(total, axis=-1, keepdims=True)).astype(jnp.bfloat16)


def attend_last(where, queries, front, back, blocks, offsets, state, text_rows):
    rows, width = queries.shape
    n_seq = len(offsets) + 1
    whole = lambda a: pl.BlockSpec(a.shape, lambda i, w: (0, 0))
    text_spec = pl.BlockSpec((text_rows, 2 * width), lambda i, w: (rows // text_rows, 0))
    return pl.pallas_call(
        functools.partial(last_kernel, offsets, rows),
        grid_spec=pltpu.PrefetchScalarGridSpec(
            num_scalar_prefetch=1,
            grid=(1,),
            in_specs=[whole(queries), whole(front), whole(back)]
            + [text_spec] * len(blocks)
            + [whole(queries)] * 2,
            out_specs=pl.BlockSpec((rows, width), lambda i, w: (0, 0)),
            scratch_shapes=[
                pltpu.VMEM((rows, 2 * width), jnp.bfloat16),
                pltpu.VMEM((n_seq * text_rows, 2 * width), jnp.bfloat16),
            ],
        ),
        out_shape=jax.ShapeDtypeStruct((rows, width), jnp.bfloat16),
        cost_estimate=pl.CostEstimate(flops=32 * rows * rows * width, bytes_accessed=8 * rows * width, transcendentals=0),
        compiler_params=pltpu.CompilerParams(vmem_limit_bytes=40 << 20),
        name="attend_last",
    )(where, queries, front, back, *blocks, *state)


def out_kernel(n_parts, x_ref, own_ref, other_ref, w_ref, coef_ref, *refs):
    outs, scratch = refs[:n_parts], refs[n_parts]
    w = w_ref[...]
    scratch[...] = coef_ref[0:1, :] * dot(own_ref[...], w) + coef_ref[1:2, :] * dot(other_ref[...], w)
    piece = outs[0].shape[0]
    for k, out in enumerate(outs):
        part = lax.rem(x_ref[0] + k, n_parts)
        rows = scratch[pl.ds(pl.multiple_of(part * piece, piece), piece), :]
        out[...] = rows.astype(out.dtype)


def out_parts(x, own, other, w_out, coef, n_parts):
    rows, width = own.shape
    cols = w_out.shape[1]
    piece = rows // n_parts
    vmem = pl.BlockSpec(memory_space=pltpu.VMEM)
    return pl.pallas_call(
        functools.partial(out_kernel, n_parts),
        in_specs=[pl.BlockSpec(memory_space=pltpu.SMEM)] + [vmem] * 4,
        out_specs=(vmem,) * n_parts,
        out_shape=tuple(
            jax.ShapeDtypeStruct((piece, cols), jnp.float32 if k == 0 else jnp.bfloat16) for k in range(n_parts)
        ),
        scratch_shapes=[pltpu.VMEM((rows, cols), jnp.float32)],
        cost_estimate=pl.CostEstimate(flops=4 * rows * width * cols, bytes_accessed=2 * width * cols, transcendentals=0),
        compiler_params=pltpu.CompilerParams(vmem_limit_bytes=40 << 20),
        name="out",
    )(x, own, other, w_out, coef)


def local(latent, positions, text_kv, text_len, modulation, w_qkv, norm_gains, w_out, guidance):
    rows = latent.shape[0]
    n_seq, n_tensor = lax.axis_size("seq"), lax.axis_size("tensor")
    text_rows = text_kv.shape[2]
    c = lax.axis_index("cfg").astype(jnp.int32)
    z = lax.axis_index("seq").astype(jnp.int32)
    x = lax.axis_index("tensor").astype(jnp.int32)
    branch = c[None]
    w_other = shifted(w_qkv, "cfg", 1)
    own_mod = lax.dynamic_index_in_dim(modulation, c, 1, keepdims=False)
    xm = modulate(latent, own_mod[:2] + jnp.array([[0.0], [1.0]], jnp.float32))
    tables = rotary_tables(positions)
    kv = keys_values(branch, xm, w_qkv, w_other, text_kv, norm_gains, tables)
    front, back = kv, kv
    blocks, offsets, state = [kv], [0], None
    queries = query_rows(branch, xm, w_qkv, w_other, norm_gains, tables)
    half = n_seq // 2
    news = [kv]
    for step in range(1, half):
        front, back = shifted(front, "seq", 1), shifted(back, "seq", -1)
        state = attend_step(queries, news, state)
        news = [front, back]
        blocks += news
        offsets += [-step, step]
    cut = rows // 2
    front, back = shifted(front[:cut], "seq", 1), shifted(back[cut:], "seq", -1)
    state = attend_step(queries, news, state)
    where = jnp.stack([z, text_len[0], jnp.int32(n_seq)])
    attended = attend_last(where, queries, front, back, blocks, tuple(offsets), state, text_rows)
    other = shifted(attended, "cfg", 1)
    cols = w_out.shape[1]
    gate = lax.dynamic_slice_in_dim(modulation[2], c * cols, cols, 1)
    strength = guidance[0]
    share = jnp.stack([strength, 1.0 - strength])[:, None] * gate
    coef = jnp.where(c == 0, share, share[::-1])
    parts = out_parts(x[None], attended, other, w_out, coef, n_tensor)
    total = parts[0]
    for k in range(1, n_tensor):
        total = total + shifted(parts[k], "tensor", k).astype(jnp.float32)
    return total.astype(jnp.bfloat16)


def solution(mesh):
    placed = (
        P(("groups", "seq"), None),
        P(None, ("groups", "seq")),
        P("cfg", None, ("groups", "seq"), "tensor"),
        P(("groups", "cfg")),
        P(None, "groups", None),
        P(None, "cfg", "tensor"),
        P(),
        P("tensor", "cfg"),
        P("groups"),
    )
    return jax.shard_map(
        local,
        mesh=mesh,
        in_specs=placed,
        out_specs=P(("groups", "seq", "tensor"), "cfg"),
        check_vma=False,
    )
```

```python
import functools
import math

import jax
import jax.numpy as jnp
import numpy as np
from jax import lax
from jax.experimental import pallas as pl
from jax.experimental.pallas import tpu as pltpu
from jax.sharding import PartitionSpec as P

HEAD_DIM = 128
EPS = 1e-06


def shifted(value, axis, by):
    n = lax.axis_size(axis)
    return lax.ppermute(value, axis, [(i, (i + by) % n) for i in range(n)])


def rotary_tables(positions):
    blocks = (HEAD_DIM // 8, 7 * HEAD_DIM // 16, 7 * HEAD_DIM // 16)
    freq = np.zeros((3, HEAD_DIM), np.float32)
    from_right = np.zeros((2, HEAD_DIM), np.float32)
    from_left = np.zeros((2, HEAD_DIM), np.float32)
    offset = 0
    for axis_id, width in enumerate(blocks):
        half = width // 2
        kind = 0 if axis_id == 0 else 1
        own = np.float32(256.0) ** (-np.arange(half, dtype=np.float32) / np.float32(half))
        freq[axis_id, offset : offset + half] = own
        freq[axis_id, offset + half : offset + width] = own
        from_right[kind, offset : offset + half] = -1.0
        from_left[kind, offset + half : offset + width] = 1.0
        offset += width
    where = positions.astype(jnp.float32)
    angle = sum(where[a][:, None] * freq[a][None, :] for a in range(3))
    cosine, sine = jnp.cos(angle), jnp.sin(angle)
    return jnp.concatenate(
        [cosine, sine * from_right[0], sine * from_left[0], sine * from_right[1], sine * from_left[1]],
        axis=1,
    )


def head_norm(heads_in, gain):
    return heads_in * lax.rsqrt(jnp.mean(heads_in * heads_in, axis=-1, keepdims=True) + EPS) * gain


def rotate(x, tables):
    d = HEAD_DIM
    small, large = d // 16, 7 * d // 32
    parts = [tables[:, i * d : (i + 1) * d] for i in range(5)]
    return (
        x * parts[0]
        + pltpu.roll(x, d - small, 1) * parts[1]
        + pltpu.roll(x, small, 1) * parts[2]
        + pltpu.roll(x, d - large, 1) * parts[3]
        + pltpu.roll(x, large, 1) * parts[4]
    )


def norm_kernel(x_ref, mod_ref, out_ref):
    x = x_ref[...].astype(jnp.float32)
    center = x - jnp.mean(x, axis=-1, keepdims=True)
    normed = center * lax.rsqrt(jnp.mean(center * center, axis=-1, keepdims=True) + EPS)
    out_ref[...] = (normed * mod_ref[1:2, :] + mod_ref[0:1, :]).astype(jnp.bfloat16)


def modulate(latent, mod):
    rows, width = latent.shape
    step = 64
    return pl.pallas_call(
        norm_kernel,
        grid=(rows // step,),
        in_specs=[
            pl.BlockSpec((step, width), lambda i: (i, 0)),
            pl.BlockSpec((2, width), lambda i: (0, 0)),
        ],
        out_specs=pl.BlockSpec((step, width), lambda i: (i, 0)),
        out_shape=jax.ShapeDtypeStruct((rows, width), jnp.bfloat16),
        cost_estimate=pl.CostEstimate(flops=3000000000, bytes_accessed=3 * rows * width, transcendentals=0),
        name="norm",
    )(latent, mod)


def dot(a, b):
    return jnp.dot(a, b, preferred_element_type=jnp.float32)


def keys_kernel(c_ref, xa_ref, xb_ref, wa_ref, wb_ref, text_ref, gain_ref, tab_ref, out_ref):
    j = pl.program_id(0)
    rows = xa_ref.shape[0]
    width = wa_ref.shape[2]
    y = dot(xa_ref[...], wa_ref[0]) + dot(xb_ref[...], wb_ref[0])
    text = text_ref[0, 0]

    @pl.when(j == 0)
    def _():
        gain = gain_ref[1:2, :]
        tables = tab_ref[...]
        for h in range(width // HEAD_DIM):
            cols = slice(h * HEAD_DIM, (h + 1) * HEAD_DIM)
            key = rotate(head_norm(y[:, cols], gain), tables)
            out_ref[0:rows, cols] = key.astype(jnp.bfloat16)
            prompt = head_norm(text[:, cols].astype(jnp.float32), gain)
            out_ref[rows:, cols] = prompt.astype(jnp.bfloat16)

    @pl.when(j == 1)
    def _():
        out_ref[0:rows, :] = y.astype(jnp.bfloat16)
        out_ref[rows:, :] = text


def keys_values(branch, xm, w_own, w_other, text_kv, gains, tables):
    rows = xm.shape[0]
    half, width = w_own.shape[1:]
    tile = width // 2
    text_rows = text_kv.shape[2]
    return pl.pallas_call(
        keys_kernel,
        grid_spec=pltpu.PrefetchScalarGridSpec(
            num_scalar_prefetch=1,
            grid=(2, 2),
            in_specs=[
                pl.BlockSpec((rows, half), lambda j, n, c: (0, c[0])),
                pl.BlockSpec((rows, half), lambda j, n, c: (0, 1 - c[0])),
                pl.BlockSpec((1, half, tile), lambda j, n, c: (1 + j, 0, n)),
                pl.BlockSpec((1, half, tile), lambda j, n, c: (1 + j, 0, n)),
                pl.BlockSpec((1, 1, text_rows, tile), lambda j, n, c: (0, j, 0, n)),
                pl.BlockSpec(gains.shape, lambda j, n, c: (0, 0)),
                pl.BlockSpec(tables.shape, lambda j, n, c: (0, 0)),
            ],
            out_specs=pl.BlockSpec((rows + text_rows, tile), lambda j, n, c: (0, 2 * j + n)),
        ),
        out_shape=jax.ShapeDtypeStruct((rows + text_rows, 2 * width), jnp.bfloat16),
        cost_estimate=pl.CostEstimate(flops=8 * rows * half * width, bytes_accessed=8 * half * width, transcendentals=0),
        compiler_params=pltpu.CompilerParams(vmem_limit_bytes=40 << 20),
        name="keys",
    )(branch, xm, xm, w_own, w_other, text_kv, gains, tables)


def query_kernel(c_ref, xa_ref, xb_ref, wa_ref, wb_ref, gain_ref, tab_ref, out_ref):
    width = wa_ref.shape[2]
    y = dot(xa_ref[...], wa_ref[0]) + dot(xb_ref[...], wb_ref[0])
    gain = gain_ref[0:1, :]
    tables = tab_ref[...]
    for h in range(width // HEAD_DIM):
        cols = slice(h * HEAD_DIM, (h + 1) * HEAD_DIM)
        out_ref[:, cols] = rotate(head_norm(y[:, cols], gain), tables).astype(jnp.bfloat16)


def query_rows(branch, xm, w_own, w_other, gains, tables):
    rows = xm.shape[0]
    half, width = w_own.shape[1:]
    tile = width // 2
    return pl.pallas_call(
        query_kernel,
        grid_spec=pltpu.PrefetchScalarGridSpec(
            num_scalar_prefetch=1,
            grid=(2,),
            in_specs=[
                pl.BlockSpec((rows, half), lambda n, c: (0, c[0])),
                pl.BlockSpec((rows, half), lambda n, c: (0, 1 - c[0])),
                pl.BlockSpec((1, half, tile), lambda n, c: (0, 0, n)),
                pl.BlockSpec((1, half, tile), lambda n, c: (0, 0, n)),
                pl.BlockSpec(gains.shape, lambda n, c: (0, 0)),
                pl.BlockSpec(tables.shape, lambda n, c: (0, 0)),
            ],
            out_specs=pl.BlockSpec((rows, tile), lambda n, c: (0, n)),
        ),
        out_shape=jax.ShapeDtypeStruct((rows, width), jnp.bfloat16),
        cost_estimate=pl.CostEstimate(flops=4 * rows * half * width, bytes_accessed=4 * half * width, transcendentals=0),
        compiler_params=pltpu.CompilerParams(vmem_limit_bytes=40 << 20),
        name="queries",
    )(branch, xm, xm, w_own, w_other, gains, tables)


SCALE = HEAD_DIM ** (-0.5) * math.log2(math.e)


def attend_block(query, key, value, total, accum, valid=None):
    scores = lax.dot_general(query, key, (((1,), (1,)), ((), ())), preferred_element_type=jnp.float32)
    expo = jnp.exp2(scores * SCALE)
    if valid is not None:
        expo = jnp.where(valid, expo, 0.0)
    for at in range(0, expo.shape[1], HEAD_DIM):
        total = total + expo[:, at : at + HEAD_DIM]
    accum = accum + dot(expo.astype(jnp.bfloat16), value)
    return total, accum


def step_kernel(n_blocks, first, rows, *refs):
    q_ref = refs[0]
    blocks = refs[1 : 1 + n_blocks]
    rest = refs[1 + n_blocks :]
    if first:
        sum_out, acc_out = rest
    else:
        sum_in, acc_in, sum_out, acc_out = rest
    width = q_ref.shape[1]
    for h in range(width // HEAD_DIM):
        cols = slice(h * HEAD_DIM, (h + 1) * HEAD_DIM)
        vcols = slice(width + h * HEAD_DIM, width + (h + 1) * HEAD_DIM)
        if first:
            total = jnp.zeros((q_ref.shape[0], HEAD_DIM), jnp.float32)
            accum = total
        else:
            total, accum = sum_in[:, cols], acc_in[:, cols]
        query = q_ref[:, cols]
        for block in blocks:
            total, accum = attend_block(query, block[0:rows, cols], block[0:rows, vcols], total, accum)
        sum_out[:, cols] = total
        acc_out[:, cols] = accum


def attend_step(queries, blocks, state):
    rows, width = queries.shape
    first = state is None
    shape = jax.ShapeDtypeStruct((rows, width), jnp.float32)
    args = (queries, *blocks) + (() if first else state)
    n_in = 1 + len(blocks)
    return pl.pallas_call(
        functools.partial(step_kernel, len(blocks), first, rows),
        out_shape=(shape, shape),
        in_specs=[pl.BlockSpec(memory_space=pltpu.VMEM)] * len(args),
        out_specs=(pl.BlockSpec(memory_space=pltpu.VMEM),) * 2,
        input_output_aliases={} if first else {n_in: 0, n_in + 1: 1},
        cost_estimate=pl.CostEstimate(
            flops=len(blocks) * 16 * rows * rows * width, bytes_accessed=4 * rows * width, transcendentals=0
        ),
        compiler_params=pltpu.CompilerParams(vmem_limit_bytes=40 << 20),
        name="attend",
    )(*args)


def last_kernel(offsets, rows, where_ref, q_ref, front_ref, back_ref, *rest):
    texts = rest[: len(offsets)]
    sum_in, acc_in, out_ref, block, prompt = rest[len(offsets) :]
    z, length, n_seq = where_ref[0], where_ref[1], where_ref[2]
    cut = front_ref.shape[0]
    text_rows = texts[0].shape[0]
    width = q_ref.shape[1]
    block[0:cut, :] = front_ref[...]
    block[cut:rows, :] = back_ref[0 : rows - cut, :]
    for text, offset in zip(texts, offsets):
        source = lax.rem(z + offset + n_seq, n_seq)
        prompt[pl.ds(pl.multiple_of(source * text_rows, text_rows), text_rows), :] = text[...]
    source = lax.rem(z + n_seq // 2, n_seq)
    prompt[pl.ds(pl.multiple_of(source * text_rows, text_rows), text_rows), :] = back_ref[rows - cut :, :]
    valid = lax.broadcasted_iota(jnp.int32, (rows, prompt.shape[0]), 1) < length
    for h in range(width // HEAD_DIM):
        cols = slice(h * HEAD_DIM, (h + 1) * HEAD_DIM)
        vcols = slice(width + h * HEAD_DIM, width + (h + 1) * HEAD_DIM)
        query = q_ref[:, cols]
        total, accum = sum_in[:, cols], acc_in[:, cols]
        total, accum = attend_block(query, block[:, cols], block[:, vcols], total, accum)
        total, accum = attend_block(query, prompt[:, cols], prompt[:, vcols], total, accum, valid)
        out_ref[:, cols] = (accum / jnp.sum(total, axis=-1, keepdims=True)).astype(jnp.bfloat16)


def attend_last(where, queries, front, back, blocks, offsets, state, text_rows):
    rows, width = queries.shape
    n_seq = len(offsets) + 1
    whole = lambda a: pl.BlockSpec(a.shape, lambda i, w: (0, 0))
    text_spec = pl.BlockSpec((text_rows, 2 * width), lambda i, w: (rows // text_rows, 0))
    return pl.pallas_call(
        functools.partial(last_kernel, offsets, rows),
        grid_spec=pltpu.PrefetchScalarGridSpec(
            num_scalar_prefetch=1,
            grid=(1,),
            in_specs=[whole(queries), whole(front), whole(back)]
            + [text_spec] * len(blocks)
            + [whole(queries)] * 2,
            out_specs=pl.BlockSpec((rows, width), lambda i, w: (0, 0)),
            scratch_shapes=[
                pltpu.VMEM((rows, 2 * width), jnp.bfloat16),
                pltpu.VMEM((n_seq * text_rows, 2 * width), jnp.bfloat16),
            ],
        ),
        out_shape=jax.ShapeDtypeStruct((rows, width), jnp.bfloat16),
        cost_estimate=pl.CostEstimate(flops=32 * rows * rows * width, bytes_accessed=8 * rows * width, transcendentals=0),
        compiler_params=pltpu.CompilerParams(vmem_limit_bytes=40 << 20),
        name="attend_last",
    )(where, queries, front, back, *blocks, *state)


def out_kernel(n_parts, x_ref, own_ref, other_ref, w_ref, coef_ref, *refs):
    outs, scratch = refs[:n_parts], refs[n_parts]
    w = w_ref[...]
    scratch[...] = coef_ref[0:1, :] * dot(own_ref[...], w) + coef_ref[1:2, :] * dot(other_ref[...], w)
    piece = outs[0].shape[0]
    for k, out in enumerate(outs):
        part = lax.rem(x_ref[0] + k, n_parts)
        rows = scratch[pl.ds(pl.multiple_of(part * piece, piece), piece), :]
        out[...] = rows.astype(out.dtype)


def out_parts(x, own, other, w_out, coef, n_parts):
    rows, width = own.shape
    cols = w_out.shape[1]
    piece = rows // n_parts
    vmem = pl.BlockSpec(memory_space=pltpu.VMEM)
    return pl.pallas_call(
        functools.partial(out_kernel, n_parts),
        in_specs=[pl.BlockSpec(memory_space=pltpu.SMEM)] + [vmem] * 4,
        out_specs=(vmem,) * n_parts,
        out_shape=tuple(
            jax.ShapeDtypeStruct((piece, cols), jnp.float32 if k == 0 else jnp.bfloat16) for k in range(n_parts)
        ),
        scratch_shapes=[pltpu.VMEM((rows, cols), jnp.float32)],
        cost_estimate=pl.CostEstimate(flops=4 * rows * width * cols, bytes_accessed=2 * width * cols, transcendentals=0),
        compiler_params=pltpu.CompilerParams(vmem_limit_bytes=40 << 20),
        name="out",
    )(x, own, other, w_out, coef)


def local(latent, positions, text_kv, text_len, modulation, w_qkv, norm_gains, w_out, guidance):
    rows = latent.shape[0]
    n_seq, n_tensor = lax.axis_size("seq"), lax.axis_size("tensor")
    text_rows = text_kv.shape[2]
    c = lax.axis_index("cfg").astype(jnp.int32)
    z = lax.axis_index("seq").astype(jnp.int32)
    x = lax.axis_index("tensor").astype(jnp.int32)
    branch = c[None]
    w_other = shifted(w_qkv, "cfg", 1)
    own_mod = lax.dynamic_index_in_dim(modulation, c, 1, keepdims=False)
    xm = modulate(latent, own_mod[:2] + jnp.array([[0.0], [1.0]], jnp.float32))
    tables = rotary_tables(positions)
    kv = keys_values(branch, xm, w_qkv, w_other, text_kv, norm_gains, tables)
    front, back = kv, kv
    blocks, offsets, state = [kv], [0], None
    queries = query_rows(branch, xm, w_qkv, w_other, norm_gains, tables)
    half = n_seq // 2
    news = [kv]
    for step in range(1, half):
        if step == 2:
            front, back, queries = lax.optimization_barrier((front, back, queries))
        elif step > 2:
            front, back, state = lax.optimization_barrier((front, back, state))
        front, back = shifted(front, "seq", 1), shifted(back, "seq", -1)
        if step > 1:
            state = attend_step(queries, news, state)
        news = news + [front, back] if step == 1 else [front, back]
        blocks += [front, back]
        offsets += [-step, step]
    cut = rows // 2
    front, back, state = lax.optimization_barrier((front, back, state))
    front, back = shifted(front[:cut], "seq", 1), shifted(back[cut:], "seq", -1)
    state = attend_step(queries, news, state)
    where = jnp.stack([z, text_len[0], jnp.int32(n_seq)])
    attended = attend_last(where, queries, front, back, blocks, tuple(offsets), state, text_rows)
    other = shifted(attended, "cfg", 1)
    cols = w_out.shape[1]
    gate = lax.dynamic_slice_in_dim(modulation[2], c * cols, cols, 1)
    strength = guidance[0]
    share = jnp.stack([strength, 1.0 - strength])[:, None] * gate
    coef = jnp.where(c == 0, share, share[::-1])
    parts = out_parts(x[None], attended, other, w_out, coef, n_tensor)
    total = parts[0]
    for k in range(1, n_tensor):
        total = total + shifted(parts[k], "tensor", k).astype(jnp.float32)
    return total.astype(jnp.bfloat16)


def solution(mesh):
    placed = (
        P(("groups", "seq"), None),
        P(None, ("groups", "seq")),
        P("cfg", None, ("groups", "seq"), "tensor"),
        P(("groups", "cfg")),
        P(None, "groups", None),
        P(None, "cfg", "tensor"),
        P(),
        P("tensor", "cfg"),
        P("groups"),
    )
    return jax.shard_map(
        local,
        mesh=mesh,
        in_specs=placed,
        out_specs=P(("groups", "seq", "tensor"), "cfg"),
        check_vma=False,
    )
```

```python
import functools
import math

import jax
import jax.numpy as jnp
import numpy as np
from jax import lax
from jax.experimental import pallas as pl
from jax.experimental.pallas import tpu as pltpu
from jax.sharding import PartitionSpec as P

HEAD_DIM = 128
EPS = 1e-06


def shifted(value, axis, by):
    n = lax.axis_size(axis)
    return lax.ppermute(value, axis, [(i, (i + by) % n) for i in range(n)])


POSITIONS = (33, 45, 80)


def rotary_constants():
    blocks = (HEAD_DIM // 8, 7 * HEAD_DIM // 16, 7 * HEAD_DIM // 16)
    angle = np.zeros((256, HEAD_DIM), np.float32)
    used = np.zeros((256, HEAD_DIM), bool)
    signs = np.zeros((4, HEAD_DIM), np.float32)
    offset = base = 0
    for axis_id, width in enumerate(blocks):
        half = width // 2
        kind = 0 if axis_id == 0 else 2
        freq = np.float32(256.0) ** (-np.arange(half, dtype=np.float32) / np.float32(half))
        count = POSITIONS[axis_id]
        turn = np.arange(count, dtype=np.float32)[:, None] * np.tile(freq, 2)[None, :]
        angle[base : base + count, offset : offset + width] = turn
        used[base : base + count, offset : offset + width] = True
        signs[kind, offset : offset + half] = -1.0
        signs[kind + 1, offset + half : offset + width] = 1.0
        offset += width
        base += count
    parts = []
    for values in (np.cos(angle.astype(np.float64)), np.sin(angle.astype(np.float64))):
        values = np.where(used, values, 0.0).astype(np.float32)
        high = values.astype(jnp.bfloat16)
        parts += [high, (values - high.astype(np.float32)).astype(jnp.bfloat16)]
    return np.concatenate(parts, axis=1), signs


def tables_kernel(pos_ref, turn_ref, sign_ref, out_ref):
    d = HEAD_DIM
    pos = pos_ref[...]
    row = lax.broadcasted_iota(jnp.int32, (turn_ref.shape[0], pos.shape[1]), 0)
    hot = row == pos[0:1, :]
    hot = hot | (row == pos[1:2, :] + POSITIONS[0])
    hot = hot | (row == pos[2:3, :] + (POSITIONS[0] + POSITIONS[1]))
    hot = jnp.where(hot, 1.0, 0.0).astype(jnp.bfloat16)
    y = lax.dot_general(hot, turn_ref[...], (((0,), (0,)), ((), ())), preferred_element_type=jnp.float32)
    sine = y[:, 2 * d : 3 * d] + y[:, 3 * d :]
    out_ref[:, 0:d] = y[:, 0:d] + y[:, d : 2 * d]
    for i in range(4):
        out_ref[:, (i + 1) * d : (i + 2) * d] = sine * sign_ref[i : i + 1, :]


def rotary_tables(positions):
    turn, signs = rotary_constants()
    count = positions.shape[1]
    return pl.pallas_call(
        tables_kernel,
        grid=(count // 128,),
        in_specs=[
            pl.BlockSpec((3, 128), lambda i: (0, i)),
            pl.BlockSpec(turn.shape, lambda i: (0, 0)),
            pl.BlockSpec(signs.shape, lambda i: (0, 0)),
        ],
        out_specs=pl.BlockSpec((128, 5 * HEAD_DIM), lambda i: (i, 0)),
        out_shape=jax.ShapeDtypeStruct((count, 5 * HEAD_DIM), jnp.float32),
        cost_estimate=pl.CostEstimate(flops=2000000 * count, bytes_accessed=2560 * count, transcendentals=0),
        name="tables",
    )(positions, jnp.asarray(turn), jnp.asarray(signs))


def head_norm(heads_in, gain):
    return heads_in * lax.rsqrt(jnp.mean(heads_in * heads_in, axis=-1, keepdims=True) + EPS) * gain


def rotate(x, tables):
    d = HEAD_DIM
    small, large = d // 16, 7 * d // 32
    parts = [tables[:, i * d : (i + 1) * d] for i in range(5)]
    return (
        x * parts[0]
        + pltpu.roll(x, d - small, 1) * parts[1]
        + pltpu.roll(x, small, 1) * parts[2]
        + pltpu.roll(x, d - large, 1) * parts[3]
        + pltpu.roll(x, large, 1) * parts[4]
    )


def norm_kernel(x_ref, mod_ref, out_ref):
    x = x_ref[...].astype(jnp.float32)
    center = x - jnp.mean(x, axis=-1, keepdims=True)
    normed = center * lax.rsqrt(jnp.mean(center * center, axis=-1, keepdims=True) + EPS)
    out_ref[...] = (normed * mod_ref[1:2, :] + mod_ref[0:1, :]).astype(jnp.bfloat16)


def modulate(latent, mod):
    rows, width = latent.shape
    step = 64
    return pl.pallas_call(
        norm_kernel,
        grid=(rows // step,),
        in_specs=[
            pl.BlockSpec((step, width), lambda i: (i, 0)),
            pl.BlockSpec((2, width), lambda i: (0, 0)),
        ],
        out_specs=pl.BlockSpec((step, width), lambda i: (i, 0)),
        out_shape=jax.ShapeDtypeStruct((rows, width), jnp.bfloat16),
        cost_estimate=pl.CostEstimate(flops=3000000000, bytes_accessed=3 * rows * width, transcendentals=0),
        name="norm",
    )(latent, mod)


def latent_kernel(where_ref, x_ref, out_ref):
    x = x_ref[...].astype(jnp.float32)
    center = x - jnp.mean(x, axis=-1, keepdims=True)
    normed = center * lax.rsqrt(jnp.mean(center * center, axis=-1, keepdims=True) + EPS)
    half = normed.shape[1] // 2
    mine = jnp.where(where_ref[1] == 0, normed[:, :half], normed[:, half:])
    out_ref[...] = mine.astype(jnp.bfloat16)


def latent_piece(where, latent, first_row, piece):
    width = latent.shape[1]
    return pl.pallas_call(
        latent_kernel,
        grid_spec=pltpu.PrefetchScalarGridSpec(
            num_scalar_prefetch=1,
            grid=(1,),
            in_specs=[pl.BlockSpec((piece, width), lambda i, w: (first_row // piece + w[0], 0))],
            out_specs=pl.BlockSpec((piece, width // 2), lambda i, w: (0, 0)),
        ),
        out_shape=jax.ShapeDtypeStruct((piece, width // 2), jnp.bfloat16),
        cost_estimate=pl.CostEstimate(flops=1000000, bytes_accessed=3 * piece * width, transcendentals=0),
        name="piece",
    )(where, latent)


def dot(a, b):
    return jnp.dot(a, b, preferred_element_type=jnp.float32)


def keys_kernel(c_ref, xa_ref, xb_ref, wa_ref, wb_ref, text_ref, gain_ref, tab_ref, lf_ref, lb_ref, own_ref, front_ref, back_ref):
    j = pl.program_id(0)
    width = wa_ref.shape[2]
    text_rows = text_ref.shape[2]
    piece = lf_ref.shape[0]
    sent = front_ref.shape[0] - text_rows - piece
    y = dot(xa_ref[...], wa_ref[0]) + dot(xb_ref[...], wb_ref[0])
    text = text_ref[0, 0]

    @pl.when(j == 0)
    def _():
        gain = gain_ref[1:2, :]
        tables = tab_ref[...]
        for h in range(width // HEAD_DIM):
            cols = slice(h * HEAD_DIM, (h + 1) * HEAD_DIM)
            key = rotate(head_norm(y[:, cols], gain), tables)
            own_ref[:, cols] = key.astype(jnp.bfloat16)
            prompt = head_norm(text[:, cols].astype(jnp.float32), gain)
            front_ref[sent : sent + text_rows, cols] = prompt.astype(jnp.bfloat16)

    @pl.when(j == 1)
    def _():
        own_ref[...] = y.astype(jnp.bfloat16)
        front_ref[sent : sent + text_rows, :] = text

    front_ref[0:sent, :] = own_ref[0:sent, :]
    back_ref[0 : sent + text_rows, :] = front_ref[0 : sent + text_rows, :]
    front_ref[sent + text_rows :, :] = lf_ref[...]
    back_ref[sent + text_rows :, :] = lb_ref[...]


def keys_values(branch, xm, w_own, w_other, text_kv, gains, tables, sent, front_piece, back_piece):
    rows = xm.shape[0]
    half, width = w_own.shape[1:]
    tile = width // 2
    text_rows = text_kv.shape[2]
    piece = front_piece.shape[0]
    total = sent + text_rows + piece
    part = lambda n: pl.BlockSpec((n, tile), lambda j, n, c: (0, 2 * j + n))
    shape = lambda n: jax.ShapeDtypeStruct((n, 2 * width), jnp.bfloat16)
    return pl.pallas_call(
        keys_kernel,
        grid_spec=pltpu.PrefetchScalarGridSpec(
            num_scalar_prefetch=1,
            grid=(2, 2),
            in_specs=[
                pl.BlockSpec((rows, half), lambda j, n, c: (0, c[0])),
                pl.BlockSpec((rows, half), lambda j, n, c: (0, 1 - c[0])),
                pl.BlockSpec((1, half, tile), lambda j, n, c: (1 + j, 0, n)),
                pl.BlockSpec((1, half, tile), lambda j, n, c: (1 + j, 0, n)),
                pl.BlockSpec((1, 1, text_rows, tile), lambda j, n, c: (0, j, 0, n)),
                pl.BlockSpec(gains.shape, lambda j, n, c: (0, 0)),
                pl.BlockSpec(tables.shape, lambda j, n, c: (0, 0)),
                part(piece),
                part(piece),
            ],
            out_specs=(part(rows), part(total), part(total)),
        ),
        out_shape=(shape(rows), shape(total), shape(total)),
        cost_estimate=pl.CostEstimate(flops=8 * rows * half * width, bytes_accessed=8 * half * width, transcendentals=0),
        compiler_params=pltpu.CompilerParams(vmem_limit_bytes=32 << 20),
        name="keys",
    )(branch, xm, xm, w_own, w_other, text_kv, gains, tables, front_piece, back_piece)


def query_kernel(c_ref, xa_ref, xb_ref, wa_ref, wb_ref, gain_ref, tab_ref, out_ref):
    width = wa_ref.shape[2]
    y = dot(xa_ref[...], wa_ref[0]) + dot(xb_ref[...], wb_ref[0])
    gain = gain_ref[0:1, :]
    tables = tab_ref[...]
    for h in range(width // HEAD_DIM):
        cols = slice(h * HEAD_DIM, (h + 1) * HEAD_DIM)
        out_ref[:, cols] = rotate(head_norm(y[:, cols], gain), tables).astype(jnp.bfloat16)


def query_rows(branch, xm, w_own, w_other, gains, tables):
    rows = xm.shape[0]
    half, width = w_own.shape[1:]
    tile = width // 2
    return pl.pallas_call(
        query_kernel,
        grid_spec=pltpu.PrefetchScalarGridSpec(
            num_scalar_prefetch=1,
            grid=(2,),
            in_specs=[
                pl.BlockSpec((rows, half), lambda n, c: (0, c[0])),
                pl.BlockSpec((rows, half), lambda n, c: (0, 1 - c[0])),
                pl.BlockSpec((1, half, tile), lambda n, c: (0, 0, n)),
                pl.BlockSpec((1, half, tile), lambda n, c: (0, 0, n)),
                pl.BlockSpec(gains.shape, lambda n, c: (0, 0)),
                pl.BlockSpec(tables.shape, lambda n, c: (0, 0)),
            ],
            out_specs=pl.BlockSpec((rows, tile), lambda n, c: (0, n)),
        ),
        out_shape=jax.ShapeDtypeStruct((rows, width), jnp.bfloat16),
        cost_estimate=pl.CostEstimate(flops=4 * rows * half * width, bytes_accessed=4 * half * width, transcendentals=0),
        compiler_params=pltpu.CompilerParams(vmem_limit_bytes=32 << 20),
        name="queries",
    )(branch, xm, xm, w_own, w_other, gains, tables)


SCALE = HEAD_DIM ** (-0.5) * math.log2(math.e)


def attend_block(query, key, value, total, accum, valid=None):
    scores = lax.dot_general(query, key, (((1,), (1,)), ((), ())), preferred_element_type=jnp.float32)
    expo = jnp.exp2(scores * SCALE)
    if valid is not None:
        expo = jnp.where(valid, expo, 0.0)
    for at in range(0, expo.shape[1], HEAD_DIM):
        total = total + expo[:, at : at + HEAD_DIM]
    accum = accum + dot(expo.astype(jnp.bfloat16), value)
    return total, accum


def step_kernel(n_blocks, first, rows, *refs):
    q_ref = refs[0]
    blocks = refs[1 : 1 + n_blocks]
    rest = refs[1 + n_blocks :]
    if first:
        sum_out, acc_out = rest
    else:
        sum_in, acc_in, sum_out, acc_out = rest
    width = q_ref.shape[1]
    for h in range(width // HEAD_DIM):
        cols = slice(h * HEAD_DIM, (h + 1) * HEAD_DIM)
        vcols = slice(width + h * HEAD_DIM, width + (h + 1) * HEAD_DIM)
        if first:
            total = jnp.zeros((q_ref.shape[0], HEAD_DIM), jnp.float32)
            accum = total
        else:
            total, accum = sum_in[:, cols], acc_in[:, cols]
        query = q_ref[:, cols]
        key = jnp.concatenate([block[0:rows, cols] for block in blocks], axis=0)
        value = jnp.concatenate([block[0:rows, vcols] for block in blocks], axis=0)
        total, accum = attend_block(query, key, value, total, accum)
        sum_out[:, cols] = total
        acc_out[:, cols] = accum


def attend_step(queries, blocks, state, used):
    rows, width = queries.shape
    first = state is None
    shape = jax.ShapeDtypeStruct((rows, width), jnp.float32)
    args = (queries, *blocks) + (() if first else state)
    n_in = 1 + len(blocks)
    return pl.pallas_call(
        functools.partial(step_kernel, len(blocks), first, used),
        out_shape=(shape, shape),
        in_specs=[pl.BlockSpec(memory_space=pltpu.VMEM)] * len(args),
        out_specs=(pl.BlockSpec(memory_space=pltpu.VMEM),) * 2,
        input_output_aliases={} if first else {n_in: 0, n_in + 1: 1},
        cost_estimate=pl.CostEstimate(
            flops=len(blocks) * 16 * rows * used * width, bytes_accessed=4 * rows * width, transcendentals=0
        ),
        compiler_params=pltpu.CompilerParams(vmem_limit_bytes=32 << 20),
        name="attend",
    )(*args)


def late_kernel(c_ref, xa_ref, xb_ref, ma_ref, mb_ref, wa_ref, wb_ref, gain_ref, tab_ref, q_ref, sum_in, acc_in, sum_out, acc_out, sa, sb, kv):
    t, r = pl.program_id(0), pl.program_id(1)
    tile = wa_ref.shape[2]
    count = kv.shape[0] // 2
    here = pl.ds(pl.multiple_of(r * count, count), count)

    @pl.when(t == 0)
    def _():
        for x_ref, m_ref, s_ref in ((xa_ref, ma_ref, sa), (xb_ref, mb_ref, sb)):
            normed = x_ref[here, :].astype(jnp.float32)
            s_ref[here, :] = (normed * m_ref[1:2, :] + m_ref[0:1, :]).astype(jnp.bfloat16)

    y = dot(sa[here, :], wa_ref[0]) + dot(sb[here, :], wb_ref[0])
    at = t * tile

    @pl.when(t < 2)
    def _():
        gain = gain_ref[1:2, :]
        tables = tab_ref[here, :]
        for h in range(tile // HEAD_DIM):
            key = rotate(head_norm(y[:, h * HEAD_DIM : (h + 1) * HEAD_DIM], gain), tables)
            kv[here, pl.ds(pl.multiple_of(at + h * HEAD_DIM, HEAD_DIM), HEAD_DIM)] = key.astype(jnp.bfloat16)

    @pl.when(t >= 2)
    def _():
        kv[here, pl.ds(pl.multiple_of(at, HEAD_DIM), tile)] = y.astype(jnp.bfloat16)

    @pl.when((t == 3) & (r == 1))
    def _():
        width = q_ref.shape[1]
        total_rows = kv.shape[0]
        for h in range(width // HEAD_DIM):
            cols = slice(h * HEAD_DIM, (h + 1) * HEAD_DIM)
            vcols = slice(width + h * HEAD_DIM, width + (h + 1) * HEAD_DIM)
            query = q_ref[:, cols]
            total, accum = sum_in[:, cols], acc_in[:, cols]
            for first in range(0, total_rows, 256):
                last = min(first + 256, total_rows)
                total, accum = attend_block(query, kv[first:last, cols], kv[first:last, vcols], total, accum)
            sum_out[:, cols] = total
            acc_out[:, cols] = accum


def attend_late(branch, own, other, mod, w_own, w_other, gains, tables, table_at, queries, state):
    count = own.shape[0]
    rows, width = queries.shape
    half = own.shape[1]
    tile = width // 2
    fixed = lambda a: pl.BlockSpec(a.shape, lambda t, r, c: (0, 0))
    shape = jax.ShapeDtypeStruct((rows, width), jnp.float32)
    return pl.pallas_call(
        late_kernel,
        grid_spec=pltpu.PrefetchScalarGridSpec(
            num_scalar_prefetch=1,
            grid=(4, 2),
            in_specs=[
                fixed(own),
                fixed(other),
                pl.BlockSpec((2, half), lambda t, r, c: (0, c[0])),
                pl.BlockSpec((2, half), lambda t, r, c: (0, 1 - c[0])),
                pl.BlockSpec((1, half, tile), lambda t, r, c: (1 + t // 2, 0, t % 2)),
                pl.BlockSpec((1, half, tile), lambda t, r, c: (1 + t // 2, 0, t % 2)),
                fixed(gains),
                pl.BlockSpec((count, tables.shape[1]), lambda t, r, c: (table_at // count, 0)),
                fixed(queries),
                fixed(shape),
                fixed(shape),
            ],
            out_specs=(fixed(shape), fixed(shape)),
            scratch_shapes=[
                pltpu.VMEM((count, half), jnp.bfloat16),
                pltpu.VMEM((count, half), jnp.bfloat16),
                pltpu.VMEM((count, 2 * width), jnp.bfloat16),
            ],
        ),
        out_shape=(shape, shape),
        cost_estimate=pl.CostEstimate(flops=12 * count * half * width, bytes_accessed=8 * half * width, transcendentals=0),
        compiler_params=pltpu.CompilerParams(vmem_limit_bytes=36 << 20),
        name="late",
    )(branch, own, other, mod, mod, w_own, w_other, gains, tables, queries, *state)


def last_kernel(offsets, sent, where_ref, q_ref, front_ref, back_ref, *rest):
    texts = rest[: len(offsets)]
    sum_in, acc_in, out_ref, block, prompt = rest[len(offsets) :]
    z, length, n_seq = where_ref[0], where_ref[1], where_ref[2]
    cut = front_ref.shape[0]
    text_rows = texts[0].shape[0]
    width = q_ref.shape[1]
    block[0:cut, :] = front_ref[...]
    block[cut:sent, :] = back_ref[0 : sent - cut, :]
    for text, offset in zip(texts, offsets):
        source = lax.rem(z + offset + n_seq, n_seq)
        prompt[pl.ds(pl.multiple_of(source * text_rows, text_rows), text_rows), :] = text[...]
    source = lax.rem(z + n_seq // 2, n_seq)
    prompt[pl.ds(pl.multiple_of(source * text_rows, text_rows), text_rows), :] = back_ref[sent - cut :, :]
    valid = lax.broadcasted_iota(jnp.int32, (q_ref.shape[0], prompt.shape[0]), 1) < length
    for h in range(width // HEAD_DIM):
        cols = slice(h * HEAD_DIM, (h + 1) * HEAD_DIM)
        vcols = slice(width + h * HEAD_DIM, width + (h + 1) * HEAD_DIM)
        query = q_ref[:, cols]
        total, accum = sum_in[:, cols], acc_in[:, cols]
        total, accum = attend_block(query, block[:, cols], block[:, vcols], total, accum)
        total, accum = attend_block(query, prompt[:, cols], prompt[:, vcols], total, accum, valid)
        out_ref[:, cols] = (accum / jnp.sum(total, axis=-1, keepdims=True)).astype(jnp.bfloat16)


def attend_last(where, queries, front, back, blocks, offsets, state, text_rows, sent):
    rows, width = queries.shape
    n_seq = len(offsets) + 1
    whole = lambda a: pl.BlockSpec(a.shape, lambda i, w: (0, 0))
    text_spec = pl.BlockSpec((text_rows, 2 * width), lambda i, w: (sent // text_rows, 0))
    return pl.pallas_call(
        functools.partial(last_kernel, offsets, sent),
        grid_spec=pltpu.PrefetchScalarGridSpec(
            num_scalar_prefetch=1,
            grid=(1,),
            in_specs=[whole(queries), whole(front), whole(back)]
            + [text_spec] * len(blocks)
            + [whole(queries)] * 2,
            out_specs=pl.BlockSpec((rows, width), lambda i, w: (0, 0)),
            scratch_shapes=[
                pltpu.VMEM((sent, 2 * width), jnp.bfloat16),
                pltpu.VMEM((n_seq * text_rows, 2 * width), jnp.bfloat16),
            ],
        ),
        out_shape=jax.ShapeDtypeStruct((rows, width), jnp.bfloat16),
        cost_estimate=pl.CostEstimate(flops=32 * rows * rows * width, bytes_accessed=8 * rows * width, transcendentals=0),
        compiler_params=pltpu.CompilerParams(vmem_limit_bytes=32 << 20),
        name="attend_last",
    )(where, queries, front, back, *blocks, *state)


def out_kernel(n_parts, x_ref, own_ref, other_ref, w_ref, coef_ref, *refs):
    outs, scratch = refs[:n_parts], refs[n_parts]
    w = w_ref[...]
    scratch[...] = coef_ref[0:1, :] * dot(own_ref[...], w) + coef_ref[1:2, :] * dot(other_ref[...], w)
    piece = outs[0].shape[0]
    for k, out in enumerate(outs):
        part = lax.rem(x_ref[0] + k, n_parts)
        rows = scratch[pl.ds(pl.multiple_of(part * piece, piece), piece), :]
        out[...] = rows.astype(out.dtype)


def out_parts(x, own, other, w_out, coef, n_parts):
    rows, width = own.shape
    cols = w_out.shape[1]
    piece = rows // n_parts
    vmem = pl.BlockSpec(memory_space=pltpu.VMEM)
    return pl.pallas_call(
        functools.partial(out_kernel, n_parts),
        in_specs=[pl.BlockSpec(memory_space=pltpu.SMEM)] + [vmem] * 4,
        out_specs=(vmem,) * n_parts,
        out_shape=tuple(
            jax.ShapeDtypeStruct((piece, cols), jnp.float32 if k == 0 else jnp.bfloat16) for k in range(n_parts)
        ),
        scratch_shapes=[pltpu.VMEM((rows, cols), jnp.float32)],
        cost_estimate=pl.CostEstimate(flops=4 * rows * width * cols, bytes_accessed=2 * width * cols, transcendentals=0),
        compiler_params=pltpu.CompilerParams(vmem_limit_bytes=32 << 20),
        name="out",
    )(x, own, other, w_out, coef)


def local(latent, positions, text_kv, text_len, modulation, w_qkv, norm_gains, w_out, guidance):
    rows = latent.shape[0]
    n_seq, n_tensor = lax.axis_size("seq"), lax.axis_size("tensor")
    text_rows = text_kv.shape[2]
    c = lax.axis_index("cfg").astype(jnp.int32)
    z = lax.axis_index("seq").astype(jnp.int32)
    x = lax.axis_index("tensor").astype(jnp.int32)
    branch = c[None]
    sent = rows // 2
    piece = (rows - sent) // n_tensor
    half = n_seq // 2
    ahead = 3
    w_other = shifted(w_qkv, "cfg", 1)
    lat = latent_piece(jnp.stack([x, c]), latent, sent, piece)
    fronts, backs = [lat], [lat]
    for _ in range(ahead):
        fronts.append(shifted(fronts[-1], "seq", 1))
        backs.append(shifted(backs[-1], "seq", -1))
    own_mod = lax.dynamic_index_in_dim(modulation, c, 1, keepdims=False)
    mod = own_mod[:2] + jnp.array([[0.0], [1.0]], jnp.float32)
    xm = modulate(latent, mod)
    own_tables = rotary_tables(positions)
    places = positions[None]
    while places.shape[0] < n_seq:
        places = jnp.concatenate([places, shifted(places, "seq", places.shape[0])], axis=0)
    order = []
    for step in range(1, half):
        order += [step, n_seq - step]
    order.append(half)
    places = places[:, :, sent:].reshape(n_seq, 3, n_tensor, piece)
    places = jnp.concatenate([places[r : r + 1] for r in order], axis=0)
    quarters = [
        lax.dynamic_index_in_dim(places, lax.rem(x + n_tensor - k, n_tensor), 2, keepdims=False)
        for k in range(n_tensor)
    ]
    places = jnp.stack(quarters, axis=1)
    ordered = [
        places[4 * i : 4 * i + 4].transpose(2, 1, 0, 3).reshape(3, -1) for i in range((len(order) + 3) // 4)
    ]
    tables = rotary_tables(jnp.concatenate(ordered, axis=1))
    kv, front, back = keys_values(
        branch, xm, w_qkv, w_other, text_kv, norm_gains, own_tables, sent, fronts[ahead], backs[ahead]
    )
    blocks, offsets, state = [front], [0], None
    queries = query_rows(branch, xm, w_qkv, w_other, norm_gains, own_tables)

    def spread(i):
        pieces = [fronts[2 * i + 1], backs[2 * i + 1], fronts[2 * i + 2]]
        if 2 * i + 2 < half:
            pieces.append(backs[2 * i + 2])
        mine = jnp.concatenate(pieces, axis=0)
        return [mine] + [shifted(mine, "tensor", k) for k in range(1, n_tensor)]

    def late(i, own, other, state):
        return attend_late(
            branch, own, other, mod, w_qkv, w_other, norm_gains, tables, i * 4 * n_tensor * piece, queries, state
        )

    kept = sent + text_rows
    moving = spread(0)
    pair = None
    for step in range(1, half + 1):
        if step == 1:
            send = (front, back)
        else:
            if step % 2 == 0:
                front, back, state, moving = lax.optimization_barrier((front, back, state, moving))
            else:
                front, back, state, pair = lax.optimization_barrier((front, back, state, pair))
            send = (front, back)
            if step == half:
                send = (front[: sent // 2], back[sent // 2 : kept])
            elif step + ahead > half:
                send = (front[:kept], back[:kept])
        new_front, new_back = shifted(send[0], "seq", 1), shifted(send[1], "seq", -1)
        if step == 1:
            state = attend_step(queries, [kv], None, rows)
        else:
            if step % 2 == 0:
                own = jnp.concatenate(moving, axis=0)
                pair = (own, shifted(own, "cfg", 1))
                if step < half:
                    moving = spread(step // 2)
            state = attend_step(queries, [front, back], state, sent)
            if step % 2 == 1:
                state = late(step // 2 - 1, *pair, state)
        front, back = new_front, new_back
        if step < half:
            blocks += [front, back]
            offsets += [-step, step]
            if step + ahead <= half:
                fronts.append(front[kept:])
                backs.append(back[kept:])
    state = late(half // 2 - 1, *pair, state)
    where = jnp.stack([z, text_len[0], jnp.int32(n_seq)])
    attended = attend_last(where, queries, front, back, blocks, tuple(offsets), state, text_rows, sent)
    other = shifted(attended, "cfg", 1)
    cols = w_out.shape[1]
    gate = lax.dynamic_slice_in_dim(modulation[2], c * cols, cols, 1)
    strength = guidance[0]
    share = jnp.stack([strength, 1.0 - strength])[:, None] * gate
    coef = jnp.where(c == 0, share, share[::-1])
    parts = out_parts(x[None], attended, other, w_out, coef, n_tensor)
    total = parts[0]
    for k in range(1, n_tensor):
        total = total + shifted(parts[k], "tensor", k).astype(jnp.float32)
    return total.astype(jnp.bfloat16)


def solution(mesh):
    placed = (
        P(("groups", "seq"), None),
        P(None, ("groups", "seq")),
        P("cfg", None, ("groups", "seq"), "tensor"),
        P(("groups", "cfg")),
        P(None, "groups", None),
        P(None, "cfg", "tensor"),
        P(),
        P("tensor", "cfg"),
        P("groups"),
    )
    return jax.shard_map(
        local,
        mesh=mesh,
        in_specs=placed,
        out_specs=P(("groups", "seq", "tensor"), "cfg"),
        check_vma=False,
    )
```

```python
import functools
import math

import jax
import jax.numpy as jnp
import numpy as np
from jax import lax
from jax.experimental import pallas as pl
from jax.experimental.pallas import tpu as pltpu
from jax.sharding import PartitionSpec as P

HEAD_DIM = 128
EPS = 1e-06


def shifted(value, axis, by):
    n = lax.axis_size(axis)
    return lax.ppermute(value, axis, [(i, (i + by) % n) for i in range(n)])


def dot(a, b):
    return jnp.dot(a, b, preferred_element_type=jnp.float32)


POSITIONS = (33, 45, 80)


def rotary_constants():
    blocks = (HEAD_DIM // 8, 7 * HEAD_DIM // 16, 7 * HEAD_DIM // 16)
    angle = np.zeros((256, HEAD_DIM), np.float32)
    used = np.zeros((256, HEAD_DIM), bool)
    signs = np.zeros((4, HEAD_DIM), np.float32)
    offset = base = 0
    for axis_id, width in enumerate(blocks):
        half = width // 2
        kind = 0 if axis_id == 0 else 2
        freq = np.float32(256.0) ** (-np.arange(half, dtype=np.float32) / np.float32(half))
        count = POSITIONS[axis_id]
        turn = np.arange(count, dtype=np.float32)[:, None] * np.tile(freq, 2)[None, :]
        angle[base : base + count, offset : offset + width] = turn
        used[base : base + count, offset : offset + width] = True
        signs[kind, offset : offset + half] = -1.0
        signs[kind + 1, offset + half : offset + width] = 1.0
        offset += width
        base += count
    parts = []
    for values in (np.cos(angle.astype(np.float64)), np.sin(angle.astype(np.float64))):
        values = np.where(used, values, 0.0).astype(np.float32)
        high = values.astype(jnp.bfloat16)
        parts += [high, (values - high.astype(np.float32)).astype(jnp.bfloat16)]
    return np.concatenate(parts, axis=1), signs


def table_rows(pos, turn_ref, sign_ref, out_ref):
    d = HEAD_DIM
    pos = pos.T
    lane = lax.broadcasted_iota(jnp.int32, (pos.shape[0], turn_ref.shape[0]), 1).astype(jnp.float32)
    hot = lane == pos[:, 0:1]
    hot = hot | (lane == pos[:, 1:2] + POSITIONS[0])
    hot = hot | (lane == pos[:, 2:3] + (POSITIONS[0] + POSITIONS[1]))
    y = dot(jnp.where(hot, 1.0, 0.0).astype(jnp.bfloat16), turn_ref[...])
    sine = y[:, 2 * d : 3 * d] + y[:, 3 * d :]
    out_ref[:, 0:d] = y[:, 0:d] + y[:, d : 2 * d]
    for i in range(4):
        out_ref[:, (i + 1) * d : (i + 2) * d] = sine * sign_ref[i : i + 1, :]


def padded(pos):
    return jnp.concatenate([pos, jnp.zeros((8 - pos.shape[0], pos.shape[1]), pos.dtype)], axis=0)


def tables_kernel(pos_ref, turn_ref, sign_ref, out_ref):
    table_rows(padded(pos_ref[...].astype(jnp.float32)), turn_ref, sign_ref, out_ref)


def rotary_tables(positions):
    turn, signs = rotary_constants()
    count = positions.shape[1]
    return pl.pallas_call(
        tables_kernel,
        grid=(count // 128,),
        in_specs=[
            pl.BlockSpec((3, 128), lambda i: (0, i)),
            pl.BlockSpec(turn.shape, lambda i: (0, 0)),
            pl.BlockSpec(signs.shape, lambda i: (0, 0)),
        ],
        out_specs=pl.BlockSpec((128, 5 * HEAD_DIM), lambda i: (i, 0)),
        out_shape=jax.ShapeDtypeStruct((count, 5 * HEAD_DIM), jnp.float32),
        cost_estimate=pl.CostEstimate(flops=2000000 * count, bytes_accessed=2560 * count, transcendentals=0),
        compiler_params=pltpu.CompilerParams(vmem_limit_bytes=8 << 20),
        name="tables",
    )(positions, jnp.asarray(turn), jnp.asarray(signs))


def head_norm(heads_in, gain):
    return heads_in * lax.rsqrt(jnp.mean(heads_in * heads_in, axis=-1, keepdims=True) + EPS) * gain


def rotate(x, tables):
    d = HEAD_DIM
    small, large = d // 16, 7 * d // 32
    parts = [tables[:, i * d : (i + 1) * d] for i in range(5)]
    return (
        x * parts[0]
        + pltpu.roll(x, d - small, 1) * parts[1]
        + pltpu.roll(x, small, 1) * parts[2]
        + pltpu.roll(x, d - large, 1) * parts[3]
        + pltpu.roll(x, large, 1) * parts[4]
    )


def norm_kernel(c_ref, x_ref, mod_ref, own_ref, other_ref):
    x = x_ref[...].astype(jnp.float32)
    center = x - jnp.mean(x, axis=-1, keepdims=True)
    normed = center * lax.rsqrt(jnp.mean(center * center, axis=-1, keepdims=True) + EPS)
    half = normed.shape[1] // 2
    mine = jnp.where(c_ref[0] == 0, normed[:, :half], normed[:, half:])
    for b, out_ref in ((0, own_ref), (1, other_ref)):
        out_ref[...] = (mine * mod_ref[2 * b + 1 : 2 * b + 2, :] + mod_ref[2 * b : 2 * b + 1, :]).astype(jnp.bfloat16)


def modulate(branch, latent, mod):
    rows, width = latent.shape
    half = width // 2
    step = 64
    shape = jax.ShapeDtypeStruct((rows, half), jnp.bfloat16)
    spec = pl.BlockSpec((step, half), lambda i, c: (i, 0))
    return pl.pallas_call(
        norm_kernel,
        grid_spec=pltpu.PrefetchScalarGridSpec(
            num_scalar_prefetch=1,
            grid=(rows // step,),
            in_specs=[
                pl.BlockSpec((step, width), lambda i, c: (i, 0)),
                pl.BlockSpec((4, half), lambda i, c: (0, c[0])),
            ],
            out_specs=(spec, spec),
        ),
        out_shape=(shape, shape),
        cost_estimate=pl.CostEstimate(flops=3000000000, bytes_accessed=4 * rows * width, transcendentals=0),
        compiler_params=pltpu.CompilerParams(vmem_limit_bytes=8 << 20),
        name="norm",
    )(branch, latent, mod)


def terms_kernel(own_ref, other_ref, w_ref, mine_ref, theirs_ref):
    w = w_ref[0]
    theirs_ref[...] = dot(other_ref[...], w).astype(jnp.bfloat16)
    mine_ref[...] = dot(own_ref[...], w)


def terms(own, other, w_qkv, first, count):
    rows, half = own.shape
    width = w_qkv.shape[2]
    tile = 2 * HEAD_DIM
    tiles = width // tile
    whole = pl.BlockSpec((rows, half), lambda n: (0, 0))
    part = pl.BlockSpec((rows, tile), lambda n: (0, n))
    return pl.pallas_call(
        terms_kernel,
        grid=(count * tiles,),
        in_specs=[whole, whole, pl.BlockSpec((1, half, tile), lambda n: (first + n // tiles, 0, n % tiles))],
        out_specs=(part, part),
        out_shape=(
            jax.ShapeDtypeStruct((rows, count * width), jnp.float32),
            jax.ShapeDtypeStruct((rows, count * width), jnp.bfloat16),
        ),
        cost_estimate=pl.CostEstimate(
            flops=4 * rows * half * count * width, bytes_accessed=2 * half * count * width, transcendentals=0
        ),
        compiler_params=pltpu.CompilerParams(vmem_limit_bytes=16 << 20),
        name="terms",
    )(own, other, w_qkv)


def keys_kernel(mine_ref, got_ref, text_ref, gain_ref, tab_ref, first_ref, second_ref):
    rows, width = mine_ref.shape[0], mine_ref.shape[1] // 2
    cut = second_ref.shape[0]
    gain = gain_ref[1:2, :]
    tables = tab_ref[...]
    for h in range(width // HEAD_DIM):
        cols = slice(h * HEAD_DIM, (h + 1) * HEAD_DIM)
        y = mine_ref[:, cols] + got_ref[:, cols].astype(jnp.float32)
        key = rotate(head_norm(y, gain), tables).astype(jnp.bfloat16)
        first_ref[0 : rows - cut, cols] = key[: rows - cut]
        second_ref[:, cols] = key[rows - cut :]
        prompt = head_norm(text_ref[0, 0, :, cols].astype(jnp.float32), gain)
        first_ref[rows - cut :, cols] = prompt.astype(jnp.bfloat16)
    value = (mine_ref[:, width:] + got_ref[:, width:].astype(jnp.float32)).astype(jnp.bfloat16)
    first_ref[0 : rows - cut, width:] = value[: rows - cut]
    second_ref[:, width:] = value[rows - cut :]
    first_ref[rows - cut :, width:] = text_ref[0, 1]


def keys_values(mine, got, text_kv, gains, tables, cut):
    rows, width = mine.shape
    text_rows = text_kv.shape[2]
    vmem = pl.BlockSpec(memory_space=pltpu.VMEM)
    return pl.pallas_call(
        keys_kernel,
        in_specs=[vmem] * 5,
        out_specs=(vmem, vmem),
        out_shape=(
            jax.ShapeDtypeStruct((rows - cut + text_rows, width), jnp.bfloat16),
            jax.ShapeDtypeStruct((cut, width), jnp.bfloat16),
        ),
        cost_estimate=pl.CostEstimate(flops=1000000000, bytes_accessed=8 * rows * width, transcendentals=0),
        compiler_params=pltpu.CompilerParams(vmem_limit_bytes=12 << 20),
        name="keys",
    )(mine, got, text_kv, gains, tables)


def query_kernel(mine_ref, got_ref, gain_ref, tab_ref, out_ref):
    gain = gain_ref[0:1, :]
    tables = tab_ref[...]
    for h in range(mine_ref.shape[1] // HEAD_DIM):
        cols = slice(h * HEAD_DIM, (h + 1) * HEAD_DIM)
        y = mine_ref[:, cols] + got_ref[:, cols].astype(jnp.float32)
        out_ref[:, cols] = rotate(head_norm(y, gain), tables).astype(jnp.bfloat16)


def query_rows(mine, got, gains, tables):
    vmem = pl.BlockSpec(memory_space=pltpu.VMEM)
    return pl.pallas_call(
        query_kernel,
        in_specs=[vmem] * 4,
        out_specs=vmem,
        out_shape=jax.ShapeDtypeStruct(mine.shape, jnp.bfloat16),
        cost_estimate=pl.CostEstimate(flops=1000000000, bytes_accessed=8 * mine.size, transcendentals=0),
        compiler_params=pltpu.CompilerParams(vmem_limit_bytes=8 << 20),
        name="queries",
    )(mine, got, gains, tables)


SCALE = HEAD_DIM ** (-0.5) * math.log2(math.e)


def attend_block(query, key, value, total, accum, valid=None):
    scores = lax.dot_general(query, key, (((1,), (1,)), ((), ())), preferred_element_type=jnp.float32)
    expo = jnp.exp2(scores * SCALE)
    if valid is not None:
        expo = jnp.where(valid, expo, 0.0)
    for at in range(0, expo.shape[1], HEAD_DIM):
        total = total + expo[:, at : at + HEAD_DIM]
    accum = accum + dot(expo.astype(jnp.bfloat16), value)
    return total, accum


def over_heads(width, body, each=1):
    @pl.loop(0, width // (each * HEAD_DIM))
    def _(i):
        for k in range(each):
            at = (each * i + k) * HEAD_DIM
            body(
                pl.ds(pl.multiple_of(at, HEAD_DIM), HEAD_DIM),
                pl.ds(pl.multiple_of(width + at, HEAD_DIM), HEAD_DIM),
            )


def step_kernel(n_blocks, first, used, *refs):
    q_ref = refs[0]
    blocks = refs[1 : 1 + n_blocks]
    rest = refs[1 + n_blocks :]
    if first:
        sum_out, acc_out, text_out = rest
    else:
        sum_in, acc_in, sum_out, acc_out, text_out = rest
    text_rows = blocks[0].shape[0] - used
    for i in range(0, n_blocks, 2):
        text_out[i // 2 * text_rows : (i // 2 + 1) * text_rows, :] = blocks[i][used:, :]
    rows = slice(0, used)

    def head(cols, vcols):
        if first:
            total = jnp.zeros((q_ref.shape[0], HEAD_DIM), jnp.float32)
            accum = total
        else:
            total, accum = sum_in[:, cols], acc_in[:, cols]
        for i in range(0, n_blocks, 2):
            key = jnp.concatenate([block[rows, cols] for block in blocks[i : i + 2]], axis=0)
            value = jnp.concatenate([block[rows, vcols] for block in blocks[i : i + 2]], axis=0)
            total, accum = attend_block(q_ref[:, cols], key, value, total, accum)
        sum_out[:, cols] = total
        acc_out[:, cols] = accum

    over_heads(q_ref.shape[1], head)


def attend_step(queries, blocks, state, used):
    rows, width = queries.shape
    first = state is None
    shape = jax.ShapeDtypeStruct((rows, width), jnp.float32)
    args = (queries, *blocks) + (() if first else tuple(state))
    n_in = 1 + len(blocks)
    text_rows = (blocks[0].shape[0] - used) * (len(blocks) // 2)
    return pl.pallas_call(
        functools.partial(step_kernel, len(blocks), first, used),
        out_shape=(shape, shape, jax.ShapeDtypeStruct((text_rows, 2 * width), jnp.bfloat16)),
        in_specs=[pl.BlockSpec(memory_space=pltpu.VMEM)] * len(args),
        out_specs=(pl.BlockSpec(memory_space=pltpu.VMEM),) * 3,
        input_output_aliases={} if first else {n_in: 0, n_in + 1: 1},
        cost_estimate=pl.CostEstimate(
            flops=len(blocks) * 16 * rows * used * width, bytes_accessed=4 * rows * width, transcendentals=0
        ),
        compiler_params=pltpu.CompilerParams(vmem_limit_bytes=12 << 20),
        name="attend",
    )(*args)


def last_kernel(offsets, where_ref, q_ref, first_ref, second_ref, *rest):
    texts = rest[: len(offsets)]
    sum_in, acc_in, out_ref, prompt = rest[len(offsets) :]
    z, length, n_seq = where_ref[0], where_ref[1], where_ref[2]
    cut = second_ref.shape[0]
    text_rows = first_ref.shape[0] - cut
    width = q_ref.shape[1]

    def place(offset, rows):
        source = lax.rem(z + offset + n_seq, n_seq)
        prompt[pl.ds(pl.multiple_of(source * text_rows, text_rows), text_rows), :] = rows

    for text, pair in zip(texts, offsets):
        for i, offset in enumerate(pair):
            place(offset, text[i * text_rows : (i + 1) * text_rows, :])
    place(len(offsets), first_ref[cut:, :])
    valid = lax.broadcasted_iota(jnp.int32, (q_ref.shape[0], prompt.shape[0]), 1) < length

    def head(cols, vcols):
        query = q_ref[:, cols]
        total, accum = sum_in[:, cols], acc_in[:, cols]
        key = jnp.concatenate([first_ref[0:cut, cols], second_ref[:, cols]], axis=0)
        value = jnp.concatenate([first_ref[0:cut, vcols], second_ref[:, vcols]], axis=0)
        total, accum = attend_block(query, key, value, total, accum)
        total, accum = attend_block(query, prompt[:, cols], prompt[:, vcols], total, accum, valid)
        out_ref[:, cols] = (accum / jnp.sum(total, axis=-1, keepdims=True)).astype(jnp.bfloat16)

    over_heads(width, head, 2)


def attend_last(where, queries, first, second, texts, offsets, state):
    rows, width = queries.shape
    n_seq = 2 * len(offsets)
    cut = second.shape[0]
    text_rows = first.shape[0] - cut
    whole = lambda a: pl.BlockSpec(a.shape, lambda i, w: (0, 0))
    return pl.pallas_call(
        functools.partial(last_kernel, offsets),
        grid_spec=pltpu.PrefetchScalarGridSpec(
            num_scalar_prefetch=1,
            grid=(1,),
            in_specs=[whole(queries), whole(first), whole(second)]
            + [whole(a) for a in texts]
            + [whole(queries)] * 2,
            out_specs=pl.BlockSpec((rows, width), lambda i, w: (0, 0)),
            scratch_shapes=[pltpu.VMEM((n_seq * text_rows, 2 * width), jnp.bfloat16)],
        ),
        out_shape=jax.ShapeDtypeStruct((rows, width), jnp.bfloat16),
        cost_estimate=pl.CostEstimate(flops=32 * rows * rows * width, bytes_accessed=8 * rows * width, transcendentals=0),
        compiler_params=pltpu.CompilerParams(vmem_limit_bytes=16 << 20),
        name="attend_last",
    )(where, queries, first, second, *texts, *state)


def out_kernel(n_parts, x_ref, own_ref, other_ref, w_ref, coef_ref, *refs):
    outs, scratch = refs[:n_parts], refs[n_parts]
    w = w_ref[...]
    scratch[...] = coef_ref[0:1, :] * dot(own_ref[...], w) + coef_ref[1:2, :] * dot(other_ref[...], w)
    piece = outs[0].shape[0]
    for k, out in enumerate(outs):
        part = lax.rem(x_ref[0] + k, n_parts)
        rows = scratch[pl.ds(pl.multiple_of(part * piece, piece), piece), :]
        out[...] = rows.astype(out.dtype)


def out_parts(x, own, other, w_out, coef, n_parts):
    rows, width = own.shape
    cols = w_out.shape[1]
    piece = rows // n_parts
    vmem = pl.BlockSpec(memory_space=pltpu.VMEM)
    return pl.pallas_call(
        functools.partial(out_kernel, n_parts),
        in_specs=[pl.BlockSpec(memory_space=pltpu.SMEM)] + [vmem] * 4,
        out_specs=(vmem,) * n_parts,
        out_shape=tuple(
            jax.ShapeDtypeStruct((piece, cols), jnp.float32 if k == 0 else jnp.bfloat16) for k in range(n_parts)
        ),
        scratch_shapes=[pltpu.VMEM((rows, cols), jnp.float32)],
        cost_estimate=pl.CostEstimate(flops=4 * rows * width * cols, bytes_accessed=2 * width * cols, transcendentals=0),
        compiler_params=pltpu.CompilerParams(vmem_limit_bytes=16 << 20),
        name="out",
    )(x, own, other, w_out, coef)


def local(latent, positions, text_kv, text_len, modulation, w_qkv, norm_gains, w_out, guidance):
    rows = latent.shape[0]
    n_seq, n_tensor = lax.axis_size("seq"), lax.axis_size("tensor")
    text_rows = text_kv.shape[2]
    c = lax.axis_index("cfg").astype(jnp.int32)
    z = lax.axis_index("seq").astype(jnp.int32)
    x = lax.axis_index("tensor").astype(jnp.int32)
    branch = c[None]
    half = n_seq // 2
    cut = rows // 2
    add = jnp.array([[0.0], [1.0]], jnp.float32)
    mod = modulation[:2] + add[:, :, None]
    own_mod = lax.dynamic_index_in_dim(mod, c, 1, keepdims=False)
    other_mod = lax.dynamic_index_in_dim(mod, 1 - c, 1, keepdims=False)
    own, other = modulate(branch, latent, jnp.concatenate([own_mod, other_mod], axis=0))
    kv_mine, kv_theirs = terms(own, other, w_qkv, 1, 2)
    kv_got = shifted(kv_theirs, "cfg", 1)
    where = jnp.stack([z, text_len[0], jnp.int32(n_seq)])
    cols = w_out.shape[1]
    gate = lax.dynamic_slice_in_dim(modulation[2], c * cols, cols, 1)
    strength = guidance[0]
    share = jnp.stack([strength, 1.0 - strength])[:, None] * gate
    coef = jnp.where(c == 0, share, share[::-1])
    kv_mine, where, coef = lax.optimization_barrier((kv_mine, where, coef))
    tables = rotary_tables(positions)
    first, second = keys_values(kv_mine, kv_got, text_kv, norm_gains, tables, cut)
    q_mine, q_theirs = terms(own, other, w_qkv, 0, 1)
    queries = query_rows(q_mine, shifted(q_theirs, "cfg", 1), norm_gains, tables)
    texts, offsets, state = [], [], None
    ahead = behind = (first, second)
    for step in range(1, half + 1):
        if step > 1:
            front, back, state = lax.optimization_barrier((ahead[0], behind[0], state))
            ahead, behind = (front, ahead[1]), (back, behind[1])
        if step < half:
            new_ahead = tuple(shifted(a, "seq", 1) for a in ahead)
            new_behind = tuple(shifted(a, "seq", -1) for a in behind)
        else:
            new_ahead = (shifted(ahead[0], "seq", 1),)
            new_behind = (shifted(behind[1], "seq", -1),)
        *state, text = attend_step(queries, ahead if step == 1 else (*ahead, *behind), state, cut)
        texts.append(text)
        offsets.append((0,) if step == 1 else (1 - step, step - 1))
        ahead, behind = new_ahead, new_behind
    attended = attend_last(where, queries, ahead[0], behind[0], texts, tuple(offsets), state)
    other = shifted(attended, "cfg", 1)
    parts = out_parts(x[None], attended, other, w_out, coef, n_tensor)
    total = parts[0]
    for k in range(1, n_tensor):
        total = total + shifted(parts[k], "tensor", k).astype(jnp.float32)
    return total.astype(jnp.bfloat16)


def solution(mesh):
    placed = (
        P(("groups", "seq"), None),
        P(None, ("groups", "seq")),
        P("cfg", None, ("groups", "seq"), "tensor"),
        P(("groups", "cfg")),
        P(None, "groups", None),
        P(None, "cfg", "tensor"),
        P(),
        P("tensor", "cfg"),
        P("groups"),
    )
    return jax.shard_map(
        local,
        mesh=mesh,
        in_specs=placed,
        out_specs=P(("groups", "seq", "tensor"), "cfg"),
        check_vma=False,
    )
```

```python
import functools
import math

import jax
import jax.numpy as jnp
import numpy as np
from jax import lax
from jax.experimental import pallas as pl
from jax.experimental.pallas import tpu as pltpu
from jax.sharding import PartitionSpec as P


HEAD_DIM = 128
EPS = 1e-06


def shifted(value, axis, by):
    n = lax.axis_size(axis)
    return lax.ppermute(value, axis, [(i, (i + by) % n) for i in range(n)])


def dot(a, b):
    return jnp.dot(a, b, preferred_element_type=jnp.float32)


POSITIONS = (33, 45, 80)


def rotary_constants():
    blocks = (HEAD_DIM // 8, 7 * HEAD_DIM // 16, 7 * HEAD_DIM // 16)
    angle = np.zeros((256, HEAD_DIM), np.float32)
    used = np.zeros((256, HEAD_DIM), bool)
    signs = np.zeros((4, HEAD_DIM), np.float32)
    offset = base = 0
    for axis_id, width in enumerate(blocks):
        half = width // 2
        kind = 0 if axis_id == 0 else 2
        freq = np.float32(256.0) ** (-np.arange(half, dtype=np.float32) / np.float32(half))
        count = POSITIONS[axis_id]
        turn = np.arange(count, dtype=np.float32)[:, None] * np.tile(freq, 2)[None, :]
        angle[base : base + count, offset : offset + width] = turn
        used[base : base + count, offset : offset + width] = True
        signs[kind, offset : offset + half] = -1.0
        signs[kind + 1, offset + half : offset + width] = 1.0
        offset += width
        base += count
    parts = []
    for values in (np.cos(angle.astype(np.float64)), np.sin(angle.astype(np.float64))):
        values = np.where(used, values, 0.0).astype(np.float32)
        high = values.astype(jnp.bfloat16)
        parts += [high, (values - high.astype(np.float32)).astype(jnp.bfloat16)]
    return np.concatenate(parts, axis=1), signs


def table_rows(pos, turn_ref, sign_ref, out_ref):
    d = HEAD_DIM
    pos = pos.T
    lane = lax.broadcasted_iota(jnp.int32, (pos.shape[0], turn_ref.shape[0]), 1).astype(jnp.float32)
    hot = lane == pos[:, 0:1]
    hot = hot | (lane == pos[:, 1:2] + POSITIONS[0])
    hot = hot | (lane == pos[:, 2:3] + (POSITIONS[0] + POSITIONS[1]))
    y = dot(jnp.where(hot, 1.0, 0.0).astype(jnp.bfloat16), turn_ref[...])
    sine = y[:, 2 * d : 3 * d] + y[:, 3 * d :]
    out_ref[:, 0:d] = y[:, 0:d] + y[:, d : 2 * d]
    for i in range(4):
        out_ref[:, (i + 1) * d : (i + 2) * d] = sine * sign_ref[i : i + 1, :]


def padded(pos):
    return jnp.concatenate([pos, jnp.zeros((8 - pos.shape[0], pos.shape[1]), pos.dtype)], axis=0)


def tables_kernel(pos_ref, turn_ref, sign_ref, out_ref):
    table_rows(padded(pos_ref[...].astype(jnp.float32)), turn_ref, sign_ref, out_ref)


def rotary_tables(positions):
    turn, signs = rotary_constants()
    count = positions.shape[1]
    return pl.pallas_call(
        tables_kernel,
        grid=(count // 128,),
        in_specs=[
            pl.BlockSpec((3, 128), lambda i: (0, i)),
            pl.BlockSpec(turn.shape, lambda i: (0, 0)),
            pl.BlockSpec(signs.shape, lambda i: (0, 0)),
        ],
        out_specs=pl.BlockSpec((128, 5 * HEAD_DIM), lambda i: (i, 0)),
        out_shape=jax.ShapeDtypeStruct((count, 5 * HEAD_DIM), jnp.float32),
        cost_estimate=pl.CostEstimate(flops=2000000 * count, bytes_accessed=2560 * count, transcendentals=0),
        compiler_params=pltpu.CompilerParams(vmem_limit_bytes=8 << 20),
        name="tables",
    )(positions, jnp.asarray(turn), jnp.asarray(signs))


def head_norm(heads_in, gain):
    return heads_in * lax.rsqrt(jnp.mean(heads_in * heads_in, axis=-1, keepdims=True) + EPS) * gain


def rotate(x, tables):
    d = HEAD_DIM
    small, large = d // 16, 7 * d // 32
    parts = [tables[:, i * d : (i + 1) * d] for i in range(5)]
    return (
        x * parts[0]
        + pltpu.roll(x, d - small, 1) * parts[1]
        + pltpu.roll(x, small, 1) * parts[2]
        + pltpu.roll(x, d - large, 1) * parts[3]
        + pltpu.roll(x, large, 1) * parts[4]
    )


def norm_kernel(c_ref, x_ref, mod_ref, own_ref, other_ref):
    x = x_ref[...].astype(jnp.float32)
    center = x - jnp.mean(x, axis=-1, keepdims=True)
    normed = center * lax.rsqrt(jnp.mean(center * center, axis=-1, keepdims=True) + EPS)
    half = normed.shape[1] // 2
    mine = jnp.where(c_ref[0] == 0, normed[:, :half], normed[:, half:])
    for branch, out_ref in ((c_ref[0], own_ref), (1 - c_ref[0], other_ref)):
        at = pl.ds(branch, 1)
        out_ref[...] = (mine * (1.0 + mod_ref[1, at, :]) + mod_ref[0, at, :]).astype(jnp.bfloat16)


def modulate(branch, latent, mod):
    rows, width = latent.shape
    half = width // 2
    step = 64
    shape = jax.ShapeDtypeStruct((rows, half), jnp.bfloat16)
    spec = pl.BlockSpec((step, half), lambda i, c: (i, 0))
    return pl.pallas_call(
        norm_kernel,
        grid_spec=pltpu.PrefetchScalarGridSpec(
            num_scalar_prefetch=1,
            grid=(rows // step,),
            in_specs=[
                pl.BlockSpec((step, width), lambda i, c: (i, 0)),
                pl.BlockSpec((*mod.shape[:2], half), lambda i, c: (0, 0, c[0])),
            ],
            out_specs=(spec, spec),
        ),
        out_shape=(shape, shape),
        cost_estimate=pl.CostEstimate(flops=3000000000, bytes_accessed=4 * rows * width, transcendentals=0),
        compiler_params=pltpu.CompilerParams(vmem_limit_bytes=8 << 20),
        name="norm",
    )(branch, latent, mod)


def terms_kernel(own_ref, other_ref, w_ref, *refs):
    mine_ref, theirs_ref = refs[-2:]
    w = w_ref[0]
    theirs_ref[...] = dot(other_ref[...], w).astype(jnp.bfloat16)
    mine_ref[...] = dot(own_ref[...], w)


def terms(own, other, w_qkv, first, count, after=()):
    rows, half = own.shape
    width = w_qkv.shape[2]
    tile = 2 * HEAD_DIM
    tiles = width // tile
    whole = pl.BlockSpec((rows, half), lambda n: (0, 0))
    part = pl.BlockSpec((rows, tile), lambda n: (0, n))
    return pl.pallas_call(
        terms_kernel,
        grid=(count * tiles,),
        in_specs=[whole, whole, pl.BlockSpec((1, half, tile), lambda n: (first + n // tiles, 0, n % tiles))]
        + [pl.BlockSpec((16, HEAD_DIM), lambda n: (0, 0)) for _ in after],
        out_specs=(part, part),
        out_shape=(
            jax.ShapeDtypeStruct((rows, count * width), jnp.float32),
            jax.ShapeDtypeStruct((rows, count * width), jnp.bfloat16),
        ),
        cost_estimate=pl.CostEstimate(
            flops=4 * rows * half * count * width, bytes_accessed=2 * half * count * width, transcendentals=0
        ),
        compiler_params=pltpu.CompilerParams(vmem_limit_bytes=16 << 20),
        name="terms",
    )(own, other, w_qkv, *after)


def over_heads(width, body, each=1):
    @pl.loop(0, width // (each * HEAD_DIM))
    def _(i):
        for k in range(each):
            at = (each * i + k) * HEAD_DIM
            body(
                pl.ds(pl.multiple_of(at, HEAD_DIM), HEAD_DIM),
                pl.ds(pl.multiple_of(width + at, HEAD_DIM), HEAD_DIM),
            )


def keys_kernel(mine_ref, got_ref, text_ref, gain_ref, tab_ref, first_ref, second_ref):
    rows, width = mine_ref.shape[0], mine_ref.shape[1] // 2
    cut = second_ref.shape[0]
    gain = gain_ref[1:2, :]
    tables = tab_ref[...]

    def head(cols, vcols):
        y = mine_ref[:, cols] + got_ref[:, cols].astype(jnp.float32)
        key = rotate(head_norm(y, gain), tables).astype(jnp.bfloat16)
        first_ref[0 : rows - cut, cols] = key[: rows - cut]
        second_ref[:, cols] = key[rows - cut :]
        prompt = head_norm(text_ref[0, 0, :, cols].astype(jnp.float32), gain)
        first_ref[rows - cut :, cols] = prompt.astype(jnp.bfloat16)
        value = (mine_ref[:, vcols] + got_ref[:, vcols].astype(jnp.float32)).astype(jnp.bfloat16)
        first_ref[0 : rows - cut, vcols] = value[: rows - cut]
        second_ref[:, vcols] = value[rows - cut :]
        first_ref[rows - cut :, vcols] = text_ref[0, 1, :, cols]

    over_heads(width, head)


def keys_values(mine, got, text_kv, gains, tables, cut):
    rows, width = mine.shape
    text_rows = text_kv.shape[2]
    vmem = pl.BlockSpec(memory_space=pltpu.VMEM)
    return pl.pallas_call(
        keys_kernel,
        in_specs=[vmem] * 5,
        out_specs=(vmem, vmem),
        out_shape=(
            jax.ShapeDtypeStruct((rows - cut + text_rows, width), jnp.bfloat16),
            jax.ShapeDtypeStruct((cut, width), jnp.bfloat16),
        ),
        cost_estimate=pl.CostEstimate(flops=1000000000, bytes_accessed=8 * rows * width, transcendentals=0),
        compiler_params=pltpu.CompilerParams(vmem_limit_bytes=12 << 20),
        name="keys",
    )(mine, got, text_kv, gains, tables)


def query_kernel(mine_ref, got_ref, gain_ref, tab_ref, out_ref):
    gain = gain_ref[0:1, :]
    tables = tab_ref[...]

    def head(cols, _):
        y = mine_ref[:, cols] + got_ref[:, cols].astype(jnp.float32)
        out_ref[:, cols] = rotate(head_norm(y, gain), tables).astype(jnp.bfloat16)

    over_heads(mine_ref.shape[1], head)


def query_rows(mine, got, gains, tables):
    vmem = pl.BlockSpec(memory_space=pltpu.VMEM)
    return pl.pallas_call(
        query_kernel,
        in_specs=[vmem] * 4,
        out_specs=vmem,
        out_shape=jax.ShapeDtypeStruct(mine.shape, jnp.bfloat16),
        cost_estimate=pl.CostEstimate(flops=1000000000, bytes_accessed=8 * mine.size, transcendentals=0),
        compiler_params=pltpu.CompilerParams(vmem_limit_bytes=8 << 20),
        name="queries",
    )(mine, got, gains, tables)


SCALE = HEAD_DIM ** (-0.5) * math.log2(math.e)


def attend_block(query, key, value, total, accum, valid=None):
    scores = lax.dot_general(query, key, (((1,), (1,)), ((), ())), preferred_element_type=jnp.float32)
    expo = jnp.exp2(scores * SCALE)
    if valid is not None:
        expo = jnp.where(valid, expo, 0.0)
    for at in range(0, expo.shape[1], HEAD_DIM):
        total = total + expo[:, at : at + HEAD_DIM]
    accum = accum + dot(expo.astype(jnp.bfloat16), value)
    return total, accum


def step_kernel(n_blocks, first, used, *refs):
    q_ref = refs[0]
    blocks = refs[1 : 1 + n_blocks]
    rest = refs[1 + n_blocks :]
    if first:
        sum_out, acc_out, text_out = rest
    else:
        sum_in, acc_in, sum_out, acc_out, text_out = rest
    text_rows = blocks[0].shape[0] - used
    for i in range(0, n_blocks, 2):
        text_out[i // 2 * text_rows : (i // 2 + 1) * text_rows, :] = blocks[i][used:, :]
    rows = slice(0, used)

    def head(cols, vcols):
        if first:
            total = jnp.zeros((q_ref.shape[0], HEAD_DIM), jnp.float32)
            accum = total
        else:
            total, accum = sum_in[:, cols], acc_in[:, cols]
        for i in range(0, n_blocks, 2):
            key = jnp.concatenate([block[rows, cols] for block in blocks[i : i + 2]], axis=0)
            value = jnp.concatenate([block[rows, vcols] for block in blocks[i : i + 2]], axis=0)
            total, accum = attend_block(q_ref[:, cols], key, value, total, accum)
        sum_out[:, cols] = total
        acc_out[:, cols] = accum

    over_heads(q_ref.shape[1], head)


def attend_step(queries, blocks, state, used):
    rows, width = queries.shape
    first = state is None
    shape = jax.ShapeDtypeStruct((rows, width), jnp.float32)
    args = (queries, *blocks) + (() if first else tuple(state))
    n_in = 1 + len(blocks)
    text_rows = (blocks[0].shape[0] - used) * (len(blocks) // 2)
    return pl.pallas_call(
        functools.partial(step_kernel, len(blocks), first, used),
        out_shape=(shape, shape, jax.ShapeDtypeStruct((text_rows, 2 * width), jnp.bfloat16)),
        in_specs=[pl.BlockSpec(memory_space=pltpu.VMEM)] * len(args),
        out_specs=(pl.BlockSpec(memory_space=pltpu.VMEM),) * 3,
        input_output_aliases={} if first else {n_in: 0, n_in + 1: 1},
        cost_estimate=pl.CostEstimate(
            flops=len(blocks) * 16 * rows * used * width, bytes_accessed=4 * rows * width, transcendentals=0
        ),
        compiler_params=pltpu.CompilerParams(vmem_limit_bytes=12 << 20),
        name="attend",
    )(*args)


def last_kernel(offsets, z_ref, length_ref, q_ref, first_ref, second_ref, *rest):
    texts = rest[: len(offsets)]
    sum_in, acc_in, out_ref, prompt = rest[len(offsets) :]
    z, length, n_seq = z_ref[0], length_ref[0], 2 * len(offsets)
    cut = second_ref.shape[0]
    text_rows = first_ref.shape[0] - cut
    width = q_ref.shape[1]

    def place(offset, rows):
        source = lax.rem(z + offset + n_seq, n_seq)
        prompt[pl.ds(pl.multiple_of(source * text_rows, text_rows), text_rows), :] = rows

    for text, pair in zip(texts, offsets):
        for i, offset in enumerate(pair):
            place(offset, text[i * text_rows : (i + 1) * text_rows, :])
    place(len(offsets), first_ref[cut:, :])
    valid = lax.broadcasted_iota(jnp.int32, (q_ref.shape[0], prompt.shape[0]), 1) < length

    def head(cols, vcols):
        query = q_ref[:, cols]
        total, accum = sum_in[:, cols], acc_in[:, cols]
        key = jnp.concatenate([first_ref[0:cut, cols], second_ref[:, cols]], axis=0)
        value = jnp.concatenate([first_ref[0:cut, vcols], second_ref[:, vcols]], axis=0)
        total, accum = attend_block(query, key, value, total, accum)
        total, accum = attend_block(query, prompt[:, cols], prompt[:, vcols], total, accum, valid)
        out_ref[:, cols] = (accum / jnp.sum(total, axis=-1, keepdims=True)).astype(jnp.bfloat16)

    over_heads(width, head, 2)


def attend_last(z, length, queries, first, second, texts, offsets, state):
    rows, width = queries.shape
    n_seq = 2 * len(offsets)
    cut = second.shape[0]
    text_rows = first.shape[0] - cut
    whole = lambda a: pl.BlockSpec(a.shape, lambda i, z, n: (0, 0))
    return pl.pallas_call(
        functools.partial(last_kernel, offsets),
        grid_spec=pltpu.PrefetchScalarGridSpec(
            num_scalar_prefetch=2,
            grid=(1,),
            in_specs=[whole(queries), whole(first), whole(second)]
            + [whole(a) for a in texts]
            + [whole(queries)] * 2,
            out_specs=pl.BlockSpec((rows, width), lambda i, z, n: (0, 0)),
            scratch_shapes=[pltpu.VMEM((n_seq * text_rows, 2 * width), jnp.bfloat16)],
        ),
        out_shape=jax.ShapeDtypeStruct((rows, width), jnp.bfloat16),
        cost_estimate=pl.CostEstimate(flops=32 * rows * rows * width, bytes_accessed=8 * rows * width, transcendentals=0),
        compiler_params=pltpu.CompilerParams(vmem_limit_bytes=16 << 20),
        name="attend_last",
    )(z, length, queries, first, second, *texts, *state)


def out_kernel(n_parts, x_ref, c_ref, strength_ref, own_ref, other_ref, w_ref, mod_ref, *refs):
    outs, scratch = refs[:n_parts], refs[n_parts]
    tile = 2 * HEAD_DIM
    width = w_ref.shape[1]
    x, c = x_ref[0], c_ref[0]
    strength = strength_ref[0]
    mine = jnp.where(c == 0, strength, 1.0 - strength)

    @pl.loop(0, w_ref.shape[1] // tile)
    def _(i):
        cols = pl.ds(pl.multiple_of(i * tile, tile), tile)
        w = w_ref[:, cols]
        own, other = dot(own_ref[...], w), dot(other_ref[...], w)
        place = pl.ds(pl.multiple_of(c * width + i * tile, tile), tile)
        gate = mod_ref[2, pl.ds(c, 1), place]
        other_gate = mod_ref[2, pl.ds(1 - c, 1), place]
        scratch[:, cols] = mine * gate * own + (1.0 - mine) * other_gate * other

    piece = outs[0].shape[0]
    for k, out in enumerate(outs):
        part = lax.rem(x + k, n_parts)
        rows = scratch[pl.ds(pl.multiple_of(part * piece, piece), piece), :]
        out[...] = rows.astype(out.dtype)


def out_parts(x, c, strength, own, other, w_out, mod, n_parts):
    rows, width = own.shape
    cols = w_out.shape[1]
    piece = rows // n_parts
    vmem = pl.BlockSpec(memory_space=pltpu.VMEM)
    return pl.pallas_call(
        functools.partial(out_kernel, n_parts),
        in_specs=[pl.BlockSpec(memory_space=pltpu.SMEM)] * 3 + [vmem] * 4,
        out_specs=(vmem,) * n_parts,
        out_shape=tuple(
            jax.ShapeDtypeStruct((piece, cols), jnp.float32 if k == 0 else jnp.bfloat16) for k in range(n_parts)
        ),
        scratch_shapes=[pltpu.VMEM((rows, cols), jnp.float32)],
        cost_estimate=pl.CostEstimate(flops=4 * rows * width * cols, bytes_accessed=2 * width * cols, transcendentals=0),
        compiler_params=pltpu.CompilerParams(vmem_limit_bytes=16 << 20),
        name="out",
    )(x, c, strength, own, other, w_out, mod)


def block(latent, positions, text_kv, text_len, modulation, w_qkv, norm_gains, w_out, guidance):
    rows = latent.shape[0]
    n_seq, n_tensor = lax.axis_size("seq"), lax.axis_size("tensor")
    c = lax.axis_index("cfg").astype(jnp.int32)
    z = lax.axis_index("seq").astype(jnp.int32)
    x = lax.axis_index("tensor").astype(jnp.int32)
    latent, z, x, branch = lax.optimization_barrier((latent, z[None], x[None], c[None]))
    half = n_seq // 2
    cut = rows // 2
    latent, modulation, w_qkv = (
        pltpu.with_memory_space_constraint(a, pltpu.MemorySpace.HBM) for a in (latent, modulation, w_qkv)
    )
    own, other = modulate(branch, latent, modulation)
    kv_mine, kv_theirs = terms(own, other, w_qkv, 1, 2)
    kv_got = shifted(kv_theirs, "cfg", 1)
    tables = rotary_tables(positions)
    first, second = keys_values(kv_mine, kv_got, text_kv, norm_gains, tables, cut)
    q_mine, q_theirs = terms(own, other, w_qkv, 0, 1, (second,))
    queries = query_rows(q_mine, shifted(q_theirs, "cfg", 1), norm_gains, tables)
    texts, offsets, state = [], [], None
    ahead = behind = (first, second)
    for step in range(1, half + 1):
        if step > 1:
            front, back, state = lax.optimization_barrier((ahead[0], behind[0], state))
            ahead, behind = (front, ahead[1]), (back, behind[1])
        if step < half:
            new_ahead = tuple(shifted(a, "seq", 1) for a in ahead)
            new_behind = tuple(shifted(a, "seq", -1) for a in behind)
        else:
            new_ahead = (shifted(ahead[0], "seq", 1),)
            new_behind = (shifted(behind[1], "seq", -1),)
        *state, text = attend_step(queries, ahead if step == 1 else (*ahead, *behind), state, cut)
        texts.append(text)
        offsets.append((0,) if step == 1 else (1 - step, step - 1))
        ahead, behind = new_ahead, new_behind
    attended = attend_last(z, text_len, queries, ahead[0], behind[0], texts, tuple(offsets), state)
    other = shifted(attended, "cfg", 1)
    parts = out_parts(x, branch, guidance, attended, other, w_out, modulation, n_tensor)
    total = parts[0]
    for k in (2, 1, 3):
        total = total + shifted(parts[k], "tensor", k).astype(jnp.float32)
    return total.astype(jnp.bfloat16)


def solution(mesh):
    placed = (
        P(("groups", "seq"), None),
        P(None, ("groups", "seq")),
        P("cfg", None, ("groups", "seq"), "tensor"),
        P(("groups", "cfg")),
        P(None, "groups", None),
        P(None, "cfg", "tensor"),
        P(),
        P("tensor", "cfg"),
        P("groups"),
    )
    return jax.shard_map(
        block,
        mesh=mesh,
        in_specs=placed,
        out_specs=P(("groups", "seq", "tensor"), "cfg"),
        check_vma=False,
    )
```

```python
import functools
import math

import jax
import jax.numpy as jnp
import numpy as np
from jax import lax
from jax.experimental import pallas as pl
from jax.experimental.pallas import tpu as pltpu
from jax.sharding import PartitionSpec as P


HEAD_DIM = 128
EPS = 1e-06


def shifted(value, axis, by):
    n = lax.axis_size(axis)
    return lax.ppermute(value, axis, [(i, (i + by) % n) for i in range(n)])


def dot(a, b):
    return jnp.dot(a, b, preferred_element_type=jnp.float32)


POSITIONS = (33, 45, 80)


def rotary_constants():
    blocks = (HEAD_DIM // 8, 7 * HEAD_DIM // 16, 7 * HEAD_DIM // 16)
    angle = np.zeros((256, HEAD_DIM), np.float32)
    used = np.zeros((256, HEAD_DIM), bool)
    signs = np.zeros((4, HEAD_DIM), np.float32)
    offset = base = 0
    for axis_id, width in enumerate(blocks):
        half = width // 2
        kind = 0 if axis_id == 0 else 2
        freq = np.float32(256.0) ** (-np.arange(half, dtype=np.float32) / np.float32(half))
        count = POSITIONS[axis_id]
        turn = np.arange(count, dtype=np.float32)[:, None] * np.tile(freq, 2)[None, :]
        angle[base : base + count, offset : offset + width] = turn
        used[base : base + count, offset : offset + width] = True
        signs[kind, offset : offset + half] = -1.0
        signs[kind + 1, offset + half : offset + width] = 1.0
        offset += width
        base += count
    parts = []
    for values in (np.cos(angle.astype(np.float64)), np.sin(angle.astype(np.float64))):
        values = np.where(used, values, 0.0).astype(np.float32)
        high = values.astype(jnp.bfloat16)
        parts += [high, (values - high.astype(np.float32)).astype(jnp.bfloat16)]
    return np.concatenate(parts, axis=1), signs


def table_rows(pos, turn_ref, sign_ref, out_ref):
    d = HEAD_DIM
    pos = pos.T
    lane = lax.broadcasted_iota(jnp.int32, (pos.shape[0], turn_ref.shape[0]), 1).astype(jnp.float32)
    hot = lane == pos[:, 0:1]
    hot = hot | (lane == pos[:, 1:2] + POSITIONS[0])
    hot = hot | (lane == pos[:, 2:3] + (POSITIONS[0] + POSITIONS[1]))
    y = dot(jnp.where(hot, 1.0, 0.0).astype(jnp.bfloat16), turn_ref[...])
    sine = y[:, 2 * d : 3 * d] + y[:, 3 * d :]
    out_ref[:, 0:d] = y[:, 0:d] + y[:, d : 2 * d]
    for i in range(4):
        out_ref[:, (i + 1) * d : (i + 2) * d] = sine * sign_ref[i : i + 1, :]


def padded(pos):
    return jnp.concatenate([pos, jnp.zeros((8 - pos.shape[0], pos.shape[1]), pos.dtype)], axis=0)


def tables_kernel(pos_ref, turn_ref, sign_ref, out_ref):
    table_rows(padded(pos_ref[...].astype(jnp.float32)), turn_ref, sign_ref, out_ref)


def rotary_tables(positions):
    turn, signs = rotary_constants()
    count = positions.shape[1]
    return pl.pallas_call(
        tables_kernel,
        grid=(count // 128,),
        in_specs=[
            pl.BlockSpec((3, 128), lambda i: (0, i)),
            pl.BlockSpec(turn.shape, lambda i: (0, 0)),
            pl.BlockSpec(signs.shape, lambda i: (0, 0)),
        ],
        out_specs=pl.BlockSpec((128, 5 * HEAD_DIM), lambda i: (i, 0)),
        out_shape=jax.ShapeDtypeStruct((count, 5 * HEAD_DIM), jnp.float32),
        cost_estimate=pl.CostEstimate(flops=2000000 * count, bytes_accessed=2560 * count, transcendentals=0),
        compiler_params=pltpu.CompilerParams(vmem_limit_bytes=8 << 20),
        name="tables",
    )(positions, jnp.asarray(turn), jnp.asarray(signs))


def head_norm(heads_in, gain):
    return heads_in * lax.rsqrt(jnp.mean(heads_in * heads_in, axis=-1, keepdims=True) + EPS) * gain


def rotate(x, tables):
    d = HEAD_DIM
    small, large = d // 16, 7 * d // 32
    parts = [tables[:, i * d : (i + 1) * d] for i in range(5)]
    return (
        x * parts[0]
        + pltpu.roll(x, d - small, 1) * parts[1]
        + pltpu.roll(x, small, 1) * parts[2]
        + pltpu.roll(x, d - large, 1) * parts[3]
        + pltpu.roll(x, large, 1) * parts[4]
    )


def norm_kernel(c_ref, x_ref, mod_ref, out_ref):
    x = x_ref[...].astype(jnp.float32)
    center = x - jnp.mean(x, axis=-1, keepdims=True)
    normed = center * lax.rsqrt(jnp.mean(center * center, axis=-1, keepdims=True) + EPS)
    half = normed.shape[1] // 2
    mine = jnp.where(c_ref[0] == 0, normed[:, :half], normed[:, half:])
    for i, branch in enumerate((c_ref[0], 1 - c_ref[0])):
        at = pl.ds(branch, 1)
        out_ref[i] = (mine * (1.0 + mod_ref[1, at, :]) + mod_ref[0, at, :]).astype(jnp.bfloat16)


def modulate(branch, latent, mod):
    rows, width = latent.shape
    half = width // 2
    step = 64
    shape = jax.ShapeDtypeStruct((2, rows, half), jnp.bfloat16)
    spec = pl.BlockSpec((2, step, half), lambda i, c: (0, i, 0))
    return pl.pallas_call(
        norm_kernel,
        grid_spec=pltpu.PrefetchScalarGridSpec(
            num_scalar_prefetch=1,
            grid=(rows // step,),
            in_specs=[
                pl.BlockSpec((step, width), lambda i, c: (i, 0)),
                pl.BlockSpec((*mod.shape[:2], half), lambda i, c: (0, 0, c[0])),
            ],
            out_specs=spec,
        ),
        out_shape=shape,
        cost_estimate=pl.CostEstimate(flops=3000000000, bytes_accessed=4 * rows * width, transcendentals=0),
        compiler_params=pltpu.CompilerParams(vmem_limit_bytes=8 << 20),
        name="norm",
    )(branch, latent, mod)


def terms_kernel(both_ref, w_ref, *refs):
    mine_ref, theirs_ref = refs[-2:]
    rows, half = both_ref.shape[1:]
    y = dot(both_ref[...].reshape(2 * rows, half), w_ref[0])
    mine_ref[...] = y[:rows]
    theirs_ref[...] = y[rows:].astype(jnp.bfloat16)


def terms(both, w_qkv, first, count, after=()):
    rows, half = both.shape[1:]
    width = w_qkv.shape[2]
    tile = 2 * HEAD_DIM
    tiles = width // tile
    whole = pl.BlockSpec(both.shape, lambda n: (0, 0, 0))
    part = pl.BlockSpec((rows, tile), lambda n: (0, n))
    return pl.pallas_call(
        terms_kernel,
        grid=(count * tiles,),
        in_specs=[whole, pl.BlockSpec((1, half, tile), lambda n: (first + n // tiles, 0, n % tiles))]
        + [pl.BlockSpec((16, HEAD_DIM), lambda n: (0, 0)) for _ in after],
        out_specs=(part, part),
        out_shape=(
            jax.ShapeDtypeStruct((rows, count * width), jnp.float32),
            jax.ShapeDtypeStruct((rows, count * width), jnp.bfloat16),
        ),
        cost_estimate=pl.CostEstimate(
            flops=4 * rows * half * count * width, bytes_accessed=2 * half * count * width, transcendentals=0
        ),
        compiler_params=pltpu.CompilerParams(vmem_limit_bytes=16 << 20),
        name="terms",
    )(both, w_qkv, *after)


def over_heads(width, body, each=1):
    @pl.loop(0, width // (each * HEAD_DIM))
    def _(i):
        for k in range(each):
            at = (each * i + k) * HEAD_DIM
            body(
                pl.ds(pl.multiple_of(at, HEAD_DIM), HEAD_DIM),
                pl.ds(pl.multiple_of(width + at, HEAD_DIM), HEAD_DIM),
            )


def keys_kernel(mine_ref, got_ref, text_ref, gain_ref, tab_ref, first_ref, second_ref):
    rows, width = mine_ref.shape[0], mine_ref.shape[1] // 2
    cut = second_ref.shape[0]
    gain = gain_ref[1:2, :]
    tables = tab_ref[...]

    def head(cols, vcols):
        y = mine_ref[:, cols] + got_ref[:, cols].astype(jnp.float32)
        key = rotate(head_norm(y, gain), tables).astype(jnp.bfloat16)
        first_ref[0 : rows - cut, cols] = key[: rows - cut]
        second_ref[:, cols] = key[rows - cut :]
        prompt = head_norm(text_ref[0, 0, :, cols].astype(jnp.float32), gain)
        first_ref[rows - cut :, cols] = prompt.astype(jnp.bfloat16)
        value = (mine_ref[:, vcols] + got_ref[:, vcols].astype(jnp.float32)).astype(jnp.bfloat16)
        first_ref[0 : rows - cut, vcols] = value[: rows - cut]
        second_ref[:, vcols] = value[rows - cut :]
        first_ref[rows - cut :, vcols] = text_ref[0, 1, :, cols]

    over_heads(width, head)


def keys_values(mine, got, text_kv, gains, tables, cut):
    rows, width = mine.shape
    text_rows = text_kv.shape[2]
    vmem = pl.BlockSpec(memory_space=pltpu.VMEM)
    return pl.pallas_call(
        keys_kernel,
        in_specs=[vmem] * 5,
        out_specs=(vmem, vmem),
        out_shape=(
            jax.ShapeDtypeStruct((rows - cut + text_rows, width), jnp.bfloat16),
            jax.ShapeDtypeStruct((cut, width), jnp.bfloat16),
        ),
        cost_estimate=pl.CostEstimate(flops=1000000000, bytes_accessed=8 * rows * width, transcendentals=0),
        compiler_params=pltpu.CompilerParams(vmem_limit_bytes=12 << 20),
        name="keys",
    )(mine, got, text_kv, gains, tables)


def query_kernel(mine_ref, got_ref, gain_ref, tab_ref, out_ref):
    gain = gain_ref[0:1, :]
    tables = tab_ref[...]

    def head(cols, _):
        y = mine_ref[:, cols] + got_ref[:, cols].astype(jnp.float32)
        out_ref[:, cols] = rotate(head_norm(y, gain), tables).astype(jnp.bfloat16)

    over_heads(mine_ref.shape[1], head)


def query_rows(mine, got, gains, tables):
    vmem = pl.BlockSpec(memory_space=pltpu.VMEM)
    return pl.pallas_call(
        query_kernel,
        in_specs=[vmem] * 4,
        out_specs=vmem,
        out_shape=jax.ShapeDtypeStruct(mine.shape, jnp.bfloat16),
        cost_estimate=pl.CostEstimate(flops=1000000000, bytes_accessed=8 * mine.size, transcendentals=0),
        compiler_params=pltpu.CompilerParams(vmem_limit_bytes=8 << 20),
        name="queries",
    )(mine, got, gains, tables)


SCALE = HEAD_DIM ** (-0.5) * math.log2(math.e)


def attend_block(query, key, value, total, accum, valid=None):
    scores = lax.dot_general(query, key, (((1,), (1,)), ((), ())), preferred_element_type=jnp.float32)
    expo = jnp.exp2(scores * SCALE)
    if valid is not None:
        expo = jnp.where(valid, expo, 0.0)
    for at in range(0, expo.shape[1], HEAD_DIM):
        total = total + expo[:, at : at + HEAD_DIM]
    accum = accum + dot(expo.astype(jnp.bfloat16), value)
    return total, accum


def step_kernel(n_blocks, first, used, *refs):
    q_ref = refs[0]
    blocks = refs[1 : 1 + n_blocks]
    rest = refs[1 + n_blocks :]
    if first:
        sum_out, acc_out, text_out = rest
    else:
        sum_in, acc_in, sum_out, acc_out, text_out = rest
    text_rows = blocks[0].shape[0] - used
    for i in range(0, n_blocks, 2):
        text_out[i // 2 * text_rows : (i // 2 + 1) * text_rows, :] = blocks[i][used:, :]
    rows = slice(0, used)

    def head(cols, vcols):
        if first:
            total = jnp.zeros((q_ref.shape[0], HEAD_DIM), jnp.float32)
            accum = total
        else:
            total, accum = sum_in[:, cols], acc_in[:, cols]
        for i in range(0, n_blocks, 2):
            key = jnp.concatenate([block[rows, cols] for block in blocks[i : i + 2]], axis=0)
            value = jnp.concatenate([block[rows, vcols] for block in blocks[i : i + 2]], axis=0)
            total, accum = attend_block(q_ref[:, cols], key, value, total, accum)
        sum_out[:, cols] = total
        acc_out[:, cols] = accum

    over_heads(q_ref.shape[1], head)


def attend_step(queries, blocks, state, used):
    rows, width = queries.shape
    first = state is None
    shape = jax.ShapeDtypeStruct((rows, width), jnp.float32)
    args = (queries, *blocks) + (() if first else tuple(state))
    n_in = 1 + len(blocks)
    text_rows = (blocks[0].shape[0] - used) * (len(blocks) // 2)
    return pl.pallas_call(
        functools.partial(step_kernel, len(blocks), first, used),
        out_shape=(shape, shape, jax.ShapeDtypeStruct((text_rows, 2 * width), jnp.bfloat16)),
        in_specs=[pl.BlockSpec(memory_space=pltpu.VMEM)] * len(args),
        out_specs=(pl.BlockSpec(memory_space=pltpu.VMEM),) * 3,
        input_output_aliases={} if first else {n_in: 0, n_in + 1: 1},
        cost_estimate=pl.CostEstimate(
            flops=len(blocks) * 16 * rows * used * width, bytes_accessed=4 * rows * width, transcendentals=0
        ),
        compiler_params=pltpu.CompilerParams(vmem_limit_bytes=12 << 20),
        name="attend",
    )(*args)


def last_kernel(offsets, z_ref, length_ref, q_ref, first_ref, second_ref, *rest):
    texts = rest[: len(offsets)]
    sum_in, acc_in, out_ref, prompt = rest[len(offsets) :]
    z, length, n_seq = z_ref[0], length_ref[0], 2 * len(offsets)
    cut = second_ref.shape[0]
    text_rows = first_ref.shape[0] - cut
    width = q_ref.shape[1]

    def place(offset, rows):
        source = lax.rem(z + offset + n_seq, n_seq)
        prompt[pl.ds(pl.multiple_of(source * text_rows, text_rows), text_rows), :] = rows

    for text, pair in zip(texts, offsets):
        for i, offset in enumerate(pair):
            place(offset, text[i * text_rows : (i + 1) * text_rows, :])
    place(len(offsets), first_ref[cut:, :])
    valid = lax.broadcasted_iota(jnp.int32, (q_ref.shape[0], prompt.shape[0]), 1) < length

    def head(cols, vcols):
        query = q_ref[:, cols]
        total, accum = sum_in[:, cols], acc_in[:, cols]
        key = jnp.concatenate([first_ref[0:cut, cols], second_ref[:, cols]], axis=0)
        value = jnp.concatenate([first_ref[0:cut, vcols], second_ref[:, vcols]], axis=0)
        total, accum = attend_block(query, key, value, total, accum)
        total, accum = attend_block(query, prompt[:, cols], prompt[:, vcols], total, accum, valid)
        out_ref[:, cols] = (accum / jnp.sum(total, axis=-1, keepdims=True)).astype(jnp.bfloat16)

    over_heads(width, head, 2)


def attend_last(z, length, queries, first, second, texts, offsets, state):
    rows, width = queries.shape
    n_seq = 2 * len(offsets)
    cut = second.shape[0]
    text_rows = first.shape[0] - cut
    whole = lambda a: pl.BlockSpec(a.shape, lambda i, z, n: (0, 0))
    return pl.pallas_call(
        functools.partial(last_kernel, offsets),
        grid_spec=pltpu.PrefetchScalarGridSpec(
            num_scalar_prefetch=2,
            grid=(1,),
            in_specs=[whole(queries), whole(first), whole(second)]
            + [whole(a) for a in texts]
            + [whole(queries)] * 2,
            out_specs=pl.BlockSpec((rows, width), lambda i, z, n: (0, 0)),
            scratch_shapes=[pltpu.VMEM((n_seq * text_rows, 2 * width), jnp.bfloat16)],
        ),
        out_shape=jax.ShapeDtypeStruct((rows, width), jnp.bfloat16),
        cost_estimate=pl.CostEstimate(flops=32 * rows * rows * width, bytes_accessed=8 * rows * width, transcendentals=0),
        compiler_params=pltpu.CompilerParams(vmem_limit_bytes=16 << 20),
        name="attend_last",
    )(z, length, queries, first, second, *texts, *state)


def out_kernel(n_parts, x_ref, c_ref, strength_ref, own_ref, other_ref, w_ref, mod_ref, *refs):
    outs, scratch = refs[:n_parts], refs[n_parts]
    tile = 2 * HEAD_DIM
    width = w_ref.shape[1]
    x, c = x_ref[0], c_ref[0]
    strength = strength_ref[0]
    mine = jnp.where(c == 0, strength, 1.0 - strength)

    @pl.loop(0, w_ref.shape[1] // tile)
    def _(i):
        cols = pl.ds(pl.multiple_of(i * tile, tile), tile)
        w = w_ref[:, cols]
        own, other = dot(own_ref[...], w), dot(other_ref[...], w)
        place = pl.ds(pl.multiple_of(c * width + i * tile, tile), tile)
        gate = mod_ref[2, pl.ds(c, 1), place]
        other_gate = mod_ref[2, pl.ds(1 - c, 1), place]
        scratch[:, cols] = mine * gate * own + (1.0 - mine) * other_gate * other

    piece = outs[0].shape[0]
    for k, out in enumerate(outs):
        part = lax.rem(x + k, n_parts)
        rows = scratch[pl.ds(pl.multiple_of(part * piece, piece), piece), :]
        out[...] = rows.astype(out.dtype)


def out_parts(x, c, strength, own, other, w_out, mod, n_parts):
    rows, width = own.shape
    cols = w_out.shape[1]
    piece = rows // n_parts
    vmem = pl.BlockSpec(memory_space=pltpu.VMEM)
    return pl.pallas_call(
        functools.partial(out_kernel, n_parts),
        in_specs=[pl.BlockSpec(memory_space=pltpu.SMEM)] * 3 + [vmem] * 4,
        out_specs=(vmem,) * n_parts,
        out_shape=tuple(
            jax.ShapeDtypeStruct((piece, cols), jnp.float32 if k == 0 else jnp.bfloat16) for k in range(n_parts)
        ),
        scratch_shapes=[pltpu.VMEM((rows, cols), jnp.float32)],
        cost_estimate=pl.CostEstimate(flops=4 * rows * width * cols, bytes_accessed=2 * width * cols, transcendentals=0),
        compiler_params=pltpu.CompilerParams(vmem_limit_bytes=16 << 20),
        name="out",
    )(x, c, strength, own, other, w_out, mod)


def block(latent, positions, text_kv, text_len, modulation, w_qkv, norm_gains, w_out, guidance):
    rows = latent.shape[0]
    n_seq, n_tensor = lax.axis_size("seq"), lax.axis_size("tensor")
    c = lax.axis_index("cfg").astype(jnp.int32)
    z = lax.axis_index("seq").astype(jnp.int32)
    x = lax.axis_index("tensor").astype(jnp.int32)
    latent, z, x, branch = lax.optimization_barrier((latent, z[None], x[None], c[None]))
    half = n_seq // 2
    cut = rows // 2
    both = modulate(branch, latent, modulation)
    kv_mine, kv_theirs = terms(both, w_qkv, 1, 2)
    kv_got = shifted(kv_theirs, "cfg", 1)
    tables = rotary_tables(positions)
    first, second = keys_values(kv_mine, kv_got, text_kv, norm_gains, tables, cut)
    q_mine, q_theirs = terms(both, w_qkv, 0, 1, (second,))
    queries = query_rows(q_mine, shifted(q_theirs, "cfg", 1), norm_gains, tables)
    texts, offsets, state = [], [], None
    ahead = behind = (first, second)
    for step in range(1, half + 1):
        if step > 1:
            front, back, state = lax.optimization_barrier((ahead[0], behind[0], state))
            ahead, behind = (front, ahead[1]), (back, behind[1])
        if step < half:
            new_ahead = tuple(shifted(a, "seq", 1) for a in ahead)
            new_behind = tuple(shifted(a, "seq", -1) for a in behind)
        else:
            new_ahead = (shifted(ahead[0], "seq", 1),)
            new_behind = (shifted(behind[1], "seq", -1),)
        *state, text = attend_step(queries, ahead if step == 1 else (*ahead, *behind), state, cut)
        texts.append(text)
        offsets.append((0,) if step == 1 else (1 - step, step - 1))
        ahead, behind = new_ahead, new_behind
    attended = attend_last(z, text_len, queries, ahead[0], behind[0], texts, tuple(offsets), state)
    other = shifted(attended, "cfg", 1)
    parts = out_parts(x, branch, guidance, attended, other, w_out, modulation, n_tensor)
    total = parts[0]
    for k in (2, 1, 3):
        total = total + shifted(parts[k], "tensor", k).astype(jnp.float32)
    return total.astype(jnp.bfloat16)


def solution(mesh):
    placed = (
        P(("groups", "seq"), None),
        P(None, ("groups", "seq")),
        P("cfg", None, ("groups", "seq"), "tensor"),
        P(("groups", "cfg")),
        P(None, "groups", None),
        P(None, "cfg", "tensor"),
        P(),
        P("tensor", "cfg"),
        P("groups"),
    )
    return jax.shard_map(
        block,
        mesh=mesh,
        in_specs=placed,
        out_specs=P(("groups", "seq", "tensor"), "cfg"),
        check_vma=False,
    )
```

```python
import functools
import math

import jax
import jax.numpy as jnp
import numpy as np
from jax import lax
from jax.experimental import pallas as pl
from jax.experimental.pallas import tpu as pltpu
from jax.sharding import PartitionSpec as P


HEAD_DIM = 128
EPS = 1e-06


def shifted(value, axis, by):
    n = lax.axis_size(axis)
    return lax.ppermute(value, axis, [(i, (i + by) % n) for i in range(n)])


def dot(a, b):
    return jnp.dot(a, b, preferred_element_type=jnp.float32)


POSITIONS = (33, 45, 80)


def rotary_constants():
    blocks = (HEAD_DIM // 8, 7 * HEAD_DIM // 16, 7 * HEAD_DIM // 16)
    angle = np.zeros((256, HEAD_DIM), np.float32)
    used = np.zeros((256, HEAD_DIM), bool)
    signs = np.zeros((4, HEAD_DIM), np.float32)
    offset = base = 0
    for axis_id, width in enumerate(blocks):
        half = width // 2
        kind = 0 if axis_id == 0 else 2
        freq = np.float32(256.0) ** (-np.arange(half, dtype=np.float32) / np.float32(half))
        count = POSITIONS[axis_id]
        turn = np.arange(count, dtype=np.float32)[:, None] * np.tile(freq, 2)[None, :]
        angle[base : base + count, offset : offset + width] = turn
        used[base : base + count, offset : offset + width] = True
        signs[kind, offset : offset + half] = -1.0
        signs[kind + 1, offset + half : offset + width] = 1.0
        offset += width
        base += count
    parts = []
    for values in (np.cos(angle.astype(np.float64)), np.sin(angle.astype(np.float64))):
        values = np.where(used, values, 0.0).astype(np.float32)
        high = values.astype(jnp.bfloat16)
        parts += [high, (values - high.astype(np.float32)).astype(jnp.bfloat16)]
    return np.concatenate(parts, axis=1), signs


def table_rows(pos, turn_ref, sign_ref, out_ref):
    d = HEAD_DIM
    pos = pos.T
    lane = lax.broadcasted_iota(jnp.int32, (pos.shape[0], turn_ref.shape[0]), 1).astype(jnp.float32)
    hot = lane == pos[:, 0:1]
    hot = hot | (lane == pos[:, 1:2] + POSITIONS[0])
    hot = hot | (lane == pos[:, 2:3] + (POSITIONS[0] + POSITIONS[1]))
    y = dot(jnp.where(hot, 1.0, 0.0).astype(jnp.bfloat16), turn_ref[...])
    sine = y[:, 2 * d : 3 * d] + y[:, 3 * d :]
    out_ref[:, 0:d] = y[:, 0:d] + y[:, d : 2 * d]
    for i in range(4):
        out_ref[:, (i + 1) * d : (i + 2) * d] = sine * sign_ref[i : i + 1, :]


def padded(pos):
    return jnp.concatenate([pos, jnp.zeros((8 - pos.shape[0], pos.shape[1]), pos.dtype)], axis=0)


def tables_kernel(pos_ref, turn_ref, sign_ref, out_ref):
    table_rows(padded(pos_ref[...].astype(jnp.float32)), turn_ref, sign_ref, out_ref)


def rotary_tables(positions):
    turn, signs = rotary_constants()
    count = positions.shape[1]
    return pl.pallas_call(
        tables_kernel,
        grid=(count // 128,),
        in_specs=[
            pl.BlockSpec((3, 128), lambda i: (0, i)),
            pl.BlockSpec(turn.shape, lambda i: (0, 0)),
            pl.BlockSpec(signs.shape, lambda i: (0, 0)),
        ],
        out_specs=pl.BlockSpec((128, 5 * HEAD_DIM), lambda i: (i, 0)),
        out_shape=jax.ShapeDtypeStruct((count, 5 * HEAD_DIM), jnp.float32),
        cost_estimate=pl.CostEstimate(flops=2000000 * count, bytes_accessed=2560 * count, transcendentals=0),
        compiler_params=pltpu.CompilerParams(vmem_limit_bytes=8 << 20),
        name="tables",
    )(positions, jnp.asarray(turn), jnp.asarray(signs))


def head_norm(heads_in, gain):
    return heads_in * lax.rsqrt(jnp.mean(heads_in * heads_in, axis=-1, keepdims=True) + EPS) * gain


def rotate(x, tables):
    d = HEAD_DIM
    small, large = d // 16, 7 * d // 32
    parts = [tables[:, i * d : (i + 1) * d] for i in range(5)]
    return (
        x * parts[0]
        + pltpu.roll(x, d - small, 1) * parts[1]
        + pltpu.roll(x, small, 1) * parts[2]
        + pltpu.roll(x, d - large, 1) * parts[3]
        + pltpu.roll(x, large, 1) * parts[4]
    )


def norm_kernel(c_ref, x_ref, mod_ref, out_ref):
    x = x_ref[...].astype(jnp.float32)
    center = x - jnp.mean(x, axis=-1, keepdims=True)
    normed = center * lax.rsqrt(jnp.mean(center * center, axis=-1, keepdims=True) + EPS)
    half = normed.shape[1] // 2
    mine = jnp.where(c_ref[0] == 0, normed[:, :half], normed[:, half:])
    for i, branch in enumerate((c_ref[0], 1 - c_ref[0])):
        at = pl.ds(branch, 1)
        out_ref[i] = (mine * (1.0 + mod_ref[1, at, :]) + mod_ref[0, at, :]).astype(jnp.bfloat16)


def modulate(branch, latent, mod):
    rows, width = latent.shape
    half = width // 2
    step = 128
    shape = jax.ShapeDtypeStruct((2, rows, half), jnp.bfloat16)
    spec = pl.BlockSpec((2, step, half), lambda i, c: (0, i, 0))
    return pl.pallas_call(
        norm_kernel,
        grid_spec=pltpu.PrefetchScalarGridSpec(
            num_scalar_prefetch=1,
            grid=(rows // step,),
            in_specs=[
                pl.BlockSpec((step, width), lambda i, c: (i, 0)),
                pl.BlockSpec((*mod.shape[:2], half), lambda i, c: (0, 0, c[0])),
            ],
            out_specs=spec,
        ),
        out_shape=shape,
        cost_estimate=pl.CostEstimate(flops=3000000000, bytes_accessed=4 * rows * width, transcendentals=0),
        compiler_params=pltpu.CompilerParams(vmem_limit_bytes=8 << 20),
        name="norm",
    )(branch, latent, mod)


def terms_kernel(both_ref, w_ref, *refs):
    mine_ref, theirs_ref = refs[-2:]
    rows, half = both_ref.shape[1:]
    y = dot(both_ref[...].reshape(2 * rows, half), w_ref[0])
    mine_ref[...] = y[:rows]
    theirs_ref[...] = y[rows:].astype(jnp.bfloat16)


def terms(both, w_qkv, first, count, after=()):
    rows, half = both.shape[1:]
    width = w_qkv.shape[2]
    tile = 2 * HEAD_DIM
    tiles = width // tile
    whole = pl.BlockSpec(both.shape, lambda n: (0, 0, 0))
    part = pl.BlockSpec((rows, tile), lambda n: (0, n))
    return pl.pallas_call(
        terms_kernel,
        grid=(count * tiles,),
        in_specs=[whole, pl.BlockSpec((1, half, tile), lambda n: (first + n // tiles, 0, n % tiles))]
        + [pl.BlockSpec((16, HEAD_DIM), lambda n: (0, 0)) for _ in after],
        out_specs=(part, part),
        out_shape=(
            jax.ShapeDtypeStruct((rows, count * width), jnp.float32),
            jax.ShapeDtypeStruct((rows, count * width), jnp.bfloat16),
        ),
        cost_estimate=pl.CostEstimate(
            flops=4 * rows * half * count * width, bytes_accessed=2 * half * count * width, transcendentals=0
        ),
        compiler_params=pltpu.CompilerParams(vmem_limit_bytes=16 << 20),
        name="terms",
    )(both, w_qkv, *after)


def over_heads(width, body, each=1):
    @pl.loop(0, width // (each * HEAD_DIM))
    def _(i):
        for k in range(each):
            at = (each * i + k) * HEAD_DIM
            body(
                pl.ds(pl.multiple_of(at, HEAD_DIM), HEAD_DIM),
                pl.ds(pl.multiple_of(width + at, HEAD_DIM), HEAD_DIM),
            )


def keys_kernel(mine_ref, got_ref, text_ref, gain_ref, tab_ref, first_ref, second_ref):
    rows, width = mine_ref.shape[0], mine_ref.shape[1] // 2
    cut = second_ref.shape[0]
    gain = gain_ref[1:2, :]
    tables = tab_ref[...]

    def head(cols, vcols):
        y = mine_ref[:, cols] + got_ref[:, cols].astype(jnp.float32)
        key = rotate(head_norm(y, gain), tables).astype(jnp.bfloat16)
        first_ref[0 : rows - cut, cols] = key[: rows - cut]
        second_ref[:, cols] = key[rows - cut :]
        prompt = head_norm(text_ref[0, 0, :, cols].astype(jnp.float32), gain)
        first_ref[rows - cut :, cols] = prompt.astype(jnp.bfloat16)
        value = (mine_ref[:, vcols] + got_ref[:, vcols].astype(jnp.float32)).astype(jnp.bfloat16)
        first_ref[0 : rows - cut, vcols] = value[: rows - cut]
        second_ref[:, vcols] = value[rows - cut :]
        first_ref[rows - cut :, vcols] = text_ref[0, 1, :, cols]

    over_heads(width, head)


def keys_values(mine, got, text_kv, gains, tables, cut):
    rows, width = mine.shape
    text_rows = text_kv.shape[2]
    vmem = pl.BlockSpec(memory_space=pltpu.VMEM)
    return pl.pallas_call(
        keys_kernel,
        in_specs=[vmem] * 5,
        out_specs=(vmem, vmem),
        out_shape=(
            jax.ShapeDtypeStruct((rows - cut + text_rows, width), jnp.bfloat16),
            jax.ShapeDtypeStruct((cut, width), jnp.bfloat16),
        ),
        cost_estimate=pl.CostEstimate(flops=1000000000, bytes_accessed=8 * rows * width, transcendentals=0),
        compiler_params=pltpu.CompilerParams(vmem_limit_bytes=12 << 20),
        name="keys",
    )(mine, got, text_kv, gains, tables)


def query_kernel(mine_ref, got_ref, gain_ref, tab_ref, out_ref):
    gain = gain_ref[0:1, :]
    tables = tab_ref[...]

    def head(cols, _):
        y = mine_ref[:, cols] + got_ref[:, cols].astype(jnp.float32)
        out_ref[:, cols] = rotate(head_norm(y, gain), tables).astype(jnp.bfloat16)

    over_heads(mine_ref.shape[1], head)


def query_rows(mine, got, gains, tables):
    vmem = pl.BlockSpec(memory_space=pltpu.VMEM)
    return pl.pallas_call(
        query_kernel,
        in_specs=[vmem] * 4,
        out_specs=vmem,
        out_shape=jax.ShapeDtypeStruct(mine.shape, jnp.bfloat16),
        cost_estimate=pl.CostEstimate(flops=1000000000, bytes_accessed=8 * mine.size, transcendentals=0),
        compiler_params=pltpu.CompilerParams(vmem_limit_bytes=8 << 20),
        name="queries",
    )(mine, got, gains, tables)


SCALE = HEAD_DIM ** (-0.5) * math.log2(math.e)


def attend_block(query, key, value, total, accum, valid=None):
    scores = lax.dot_general(query, key, (((1,), (1,)), ((), ())), preferred_element_type=jnp.float32)
    expo = jnp.exp2(scores * SCALE)
    if valid is not None:
        expo = jnp.where(valid, expo, 0.0)
    for at in range(0, expo.shape[1], HEAD_DIM):
        total = total + expo[:, at : at + HEAD_DIM]
    accum = accum + dot(expo.astype(jnp.bfloat16), value)
    return total, accum


def step_kernel(n_blocks, first, used, *refs):
    q_ref = refs[0]
    blocks = refs[1 : 1 + n_blocks]
    rest = refs[1 + n_blocks :]
    if first:
        sum_out, acc_out, text_out = rest
    else:
        sum_in, acc_in, sum_out, acc_out, text_out = rest
    text_rows = blocks[0].shape[0] - used
    for i in range(0, n_blocks, 2):
        text_out[i // 2 * text_rows : (i // 2 + 1) * text_rows, :] = blocks[i][used:, :]
    rows = slice(0, used)

    def head(cols, vcols):
        if first:
            total = jnp.zeros((q_ref.shape[0], HEAD_DIM), jnp.float32)
            accum = total
        else:
            total, accum = sum_in[:, cols], acc_in[:, cols]
        for i in range(0, n_blocks, 2):
            key = jnp.concatenate([block[rows, cols] for block in blocks[i : i + 2]], axis=0)
            value = jnp.concatenate([block[rows, vcols] for block in blocks[i : i + 2]], axis=0)
            total, accum = attend_block(q_ref[:, cols], key, value, total, accum)
        sum_out[:, cols] = total
        acc_out[:, cols] = accum

    over_heads(q_ref.shape[1], head)


def attend_step(queries, blocks, state, used):
    rows, width = queries.shape
    first = state is None
    shape = jax.ShapeDtypeStruct((rows, width), jnp.float32)
    args = (queries, *blocks) + (() if first else tuple(state))
    n_in = 1 + len(blocks)
    text_rows = (blocks[0].shape[0] - used) * (len(blocks) // 2)
    return pl.pallas_call(
        functools.partial(step_kernel, len(blocks), first, used),
        out_shape=(shape, shape, jax.ShapeDtypeStruct((text_rows, 2 * width), jnp.bfloat16)),
        in_specs=[pl.BlockSpec(memory_space=pltpu.VMEM)] * len(args),
        out_specs=(pl.BlockSpec(memory_space=pltpu.VMEM),) * 3,
        input_output_aliases={} if first else {n_in: 0, n_in + 1: 1},
        cost_estimate=pl.CostEstimate(
            flops=len(blocks) * 16 * rows * used * width, bytes_accessed=4 * rows * width, transcendentals=0
        ),
        compiler_params=pltpu.CompilerParams(vmem_limit_bytes=12 << 20),
        name="attend",
    )(*args)


def last_kernel(offsets, z_ref, length_ref, q_ref, first_ref, second_ref, *rest):
    texts = rest[: len(offsets)]
    sum_in, acc_in, out_ref, prompt = rest[len(offsets) :]
    z, length, n_seq = z_ref[0], length_ref[0], 2 * len(offsets)
    cut = second_ref.shape[0]
    text_rows = first_ref.shape[0] - cut
    width = q_ref.shape[1]

    def place(offset, rows):
        source = lax.rem(z + offset + n_seq, n_seq)
        prompt[pl.ds(pl.multiple_of(source * text_rows, text_rows), text_rows), :] = rows

    for text, pair in zip(texts, offsets):
        for i, offset in enumerate(pair):
            place(offset, text[i * text_rows : (i + 1) * text_rows, :])
    place(len(offsets), first_ref[cut:, :])
    valid = lax.broadcasted_iota(jnp.int32, (q_ref.shape[0], prompt.shape[0]), 1) < length

    def head(cols, vcols):
        query = q_ref[:, cols]
        total, accum = sum_in[:, cols], acc_in[:, cols]
        key = jnp.concatenate([first_ref[0:cut, cols], second_ref[:, cols]], axis=0)
        value = jnp.concatenate([first_ref[0:cut, vcols], second_ref[:, vcols]], axis=0)
        total, accum = attend_block(query, key, value, total, accum)
        total, accum = attend_block(query, prompt[:, cols], prompt[:, vcols], total, accum, valid)
        out_ref[:, cols] = (accum / jnp.sum(total, axis=-1, keepdims=True)).astype(jnp.bfloat16)

    over_heads(width, head, 2)


def attend_last(z, length, queries, first, second, texts, offsets, state):
    rows, width = queries.shape
    n_seq = 2 * len(offsets)
    cut = second.shape[0]
    text_rows = first.shape[0] - cut
    whole = lambda a: pl.BlockSpec(a.shape, lambda i, z, n: (0, 0))
    return pl.pallas_call(
        functools.partial(last_kernel, offsets),
        grid_spec=pltpu.PrefetchScalarGridSpec(
            num_scalar_prefetch=2,
            grid=(1,),
            in_specs=[whole(queries), whole(first), whole(second)]
            + [whole(a) for a in texts]
            + [whole(queries)] * 2,
            out_specs=pl.BlockSpec((rows, width), lambda i, z, n: (0, 0)),
            scratch_shapes=[pltpu.VMEM((n_seq * text_rows, 2 * width), jnp.bfloat16)],
        ),
        out_shape=jax.ShapeDtypeStruct((rows, width), jnp.bfloat16),
        cost_estimate=pl.CostEstimate(flops=32 * rows * rows * width, bytes_accessed=8 * rows * width, transcendentals=0),
        compiler_params=pltpu.CompilerParams(vmem_limit_bytes=16 << 20),
        name="attend_last",
    )(z, length, queries, first, second, *texts, *state)


def out_kernel(n_parts, x_ref, c_ref, strength_ref, own_ref, other_ref, w_ref, mod_ref, *refs):
    outs, scratch = refs[:n_parts], refs[n_parts]
    tile = 2 * HEAD_DIM
    width = w_ref.shape[1]
    x, c = x_ref[0], c_ref[0]
    strength = strength_ref[0]
    mine = jnp.where(c == 0, strength, 1.0 - strength)

    @pl.loop(0, w_ref.shape[1] // tile)
    def _(i):
        cols = pl.ds(pl.multiple_of(i * tile, tile), tile)
        w = w_ref[:, cols]
        own, other = dot(own_ref[...], w), dot(other_ref[...], w)
        place = pl.ds(pl.multiple_of(c * width + i * tile, tile), tile)
        gate = mod_ref[2, pl.ds(c, 1), place]
        other_gate = mod_ref[2, pl.ds(1 - c, 1), place]
        scratch[:, cols] = mine * gate * own + (1.0 - mine) * other_gate * other

    piece = outs[0].shape[0]
    for k, out in enumerate(outs):
        part = lax.rem(x + k, n_parts)
        rows = scratch[pl.ds(pl.multiple_of(part * piece, piece), piece), :]
        out[...] = rows.astype(out.dtype)


def out_parts(x, c, strength, own, other, w_out, mod, n_parts):
    rows, width = own.shape
    cols = w_out.shape[1]
    piece = rows // n_parts
    vmem = pl.BlockSpec(memory_space=pltpu.VMEM)
    return pl.pallas_call(
        functools.partial(out_kernel, n_parts),
        in_specs=[pl.BlockSpec(memory_space=pltpu.SMEM)] * 3 + [vmem] * 4,
        out_specs=(vmem,) * n_parts,
        out_shape=tuple(
            jax.ShapeDtypeStruct((piece, cols), jnp.float32 if k == 0 else jnp.bfloat16) for k in range(n_parts)
        ),
        scratch_shapes=[pltpu.VMEM((rows, cols), jnp.float32)],
        cost_estimate=pl.CostEstimate(flops=4 * rows * width * cols, bytes_accessed=2 * width * cols, transcendentals=0),
        compiler_params=pltpu.CompilerParams(vmem_limit_bytes=16 << 20),
        name="out",
    )(x, c, strength, own, other, w_out, mod)


def block(latent, positions, text_kv, text_len, modulation, w_qkv, norm_gains, w_out, guidance):
    rows = latent.shape[0]
    n_seq, n_tensor = lax.axis_size("seq"), lax.axis_size("tensor")
    c = lax.axis_index("cfg").astype(jnp.int32)
    z = lax.axis_index("seq").astype(jnp.int32)
    x = lax.axis_index("tensor").astype(jnp.int32)
    latent, z, x, branch = lax.optimization_barrier((latent, z[None], x[None], c[None]))
    half = n_seq // 2
    cut = rows // 2
    hbm = lambda a: pltpu.with_memory_space_constraint(a, pltpu.MemorySpace.HBM)
    both = modulate(branch, hbm(latent), hbm(modulation))
    kv_mine, kv_theirs = terms(both, w_qkv, 1, 2)
    kv_got = shifted(kv_theirs, "cfg", 1)
    tables = rotary_tables(positions)
    first, second = keys_values(kv_mine, kv_got, text_kv, norm_gains, tables, cut)
    q_mine, q_theirs = terms(both, w_qkv, 0, 1, (second,))
    queries = query_rows(q_mine, shifted(q_theirs, "cfg", 1), norm_gains, tables)
    texts, offsets, state = [], [], None
    ahead = behind = (first, second)
    for step in range(1, half + 1):
        if step > 1:
            front, back, state = lax.optimization_barrier((ahead[0], behind[0], state))
            ahead, behind = (front, ahead[1]), (back, behind[1])
        if step < half:
            new_ahead = tuple(shifted(a, "seq", 1) for a in ahead)
            new_behind = tuple(shifted(a, "seq", -1) for a in behind)
        else:
            new_ahead = (shifted(ahead[0], "seq", 1),)
            new_behind = (shifted(behind[1], "seq", -1),)
        *state, text = attend_step(queries, ahead if step == 1 else (*ahead, *behind), state, cut)
        texts.append(text)
        offsets.append((0,) if step == 1 else (1 - step, step - 1))
        ahead, behind = new_ahead, new_behind
    attended = attend_last(z, text_len, queries, ahead[0], behind[0], texts, tuple(offsets), state)
    other = shifted(attended, "cfg", 1)
    parts = out_parts(x, branch, guidance, attended, other, w_out, modulation, n_tensor)
    total = parts[0]
    for k in (2, 1, 3):
        total = total + shifted(parts[k], "tensor", k).astype(jnp.float32)
    return total.astype(jnp.bfloat16)


def solution(mesh):
    placed = (
        P(("groups", "seq"), None),
        P(None, ("groups", "seq")),
        P("cfg", None, ("groups", "seq"), "tensor"),
        P(("groups", "cfg")),
        P(None, "groups", None),
        P(None, "cfg", "tensor"),
        P(),
        P("tensor", "cfg"),
        P("groups"),
    )
    return jax.shard_map(
        block,
        mesh=mesh,
        in_specs=placed,
        out_specs=P(("groups", "seq", "tensor"), "cfg"),
        check_vma=False,
    )
```
